256 devices in a mesh: grp: 2 (over y), page: 128 (over z, x, core).
Axes of the slice: x: 4, y: 2, z: 16, core: 2. Of those that a mesh axis runs over, the one named last changes fastest.
The devices are a block of a 4x16x16 slice.
Arguments:
- queries: bfloat16 [32, 4096], P('grp'), parts along dimension 0, may hold values from -64 to 64
- key_cache: bfloat16 [8192, 64, 1024], P(('grp', 'page')), parts along dimension 0, may hold values from -9 to 9
- value_cache: bfloat16 [8192, 64, 1024], P(('grp', 'page')), parts along dimension 0, may hold values from -16 to 16
- new_keys: bfloat16 [32, 1024], P('grp'), parts along dimension 0, may hold values from -16 to 16
- new_values: bfloat16 [32, 1024], P('grp'), parts along dimension 0, may hold values from -6 to 6
- chosen: int32 [16, 256], P('grp', 'page'), parts along dimension 0, may hold values from 0 to 4095, as said below
Outputs:
- attended: bfloat16 [32, 4096], P('grp'), parts along dimension 0
The draws below stay inside these ranges and needn't reach their ends.
There are 2 independent parts, one for each index of `grp`. The reference program is written for one: setup_inputs(seed, part) draws one part's arguments, and reference() takes and returns one part's arrays. A program takes and returns all parts, laid end to end along the dimension named above; each array names one. Nothing has to cross between parts.
Inputs may be any that keep to these rules, and one draw needn't show every extreme that they name: `chosen`: each row names 256 different pages; at most 8 of a row's pages lie in the range of 32 pages of one device, and exactly 8 do for some device in every row.
All inputs are finite; a program needn't handle non-finite values.
Results may differ from the reference program's by a relative error of at most 0.004.
Values may be sent and summed in bfloat16 or wider, within the bound.
A program may use at most 64 MiB of HBM per device.

```python
import jax
import jax.numpy as jnp
from jax import lax

MEMORY_GROUPS = 8
G = 4
D = 128
PAGE = 64
K = 256
PPD = 32
DRAFT = 16
CAPH = 8
N_PAGE = 128


def draw_chosen(key, part):
    overall_block_tally = PPD * N_PAGE
    key_order = jax.random.fold_in(key, 11)
    lookup_extra_rating = jax.random.fold_in(key, 12)
    key_heat = jax.random.fold_in(key, 13)
    precedence_rating = jax.vmap(lambda single: jax.random.permutation(single, overall_block_tally))(jax.random.split(key_order, MEMORY_GROUPS))
    precedence_rating = precedence_rating.astype(jnp.int32).reshape(MEMORY_GROUPS, N_PAGE, PPD)
    beaten = jnp.sum((precedence_rating[:, :, None, :] > precedence_rating[:, :, :, None]).astype(jnp.int32), axis=3)
    admissible_blocks = beaten < CAPH
    extra_lift_amount = jax.random.randint(lookup_extra_rating, (MEMORY_GROUPS, N_PAGE), 0, 4).astype(jnp.int32)
    strongest_blocks = jax.random.randint(key_heat, (MEMORY_GROUPS, 1), 0, N_PAGE).astype(jnp.int32)
    shard_identifiers = jnp.arange(N_PAGE, dtype=jnp.int32)[None, :]
    extra_lift_amount = jnp.where(shard_identifiers == strongest_blocks, 5, extra_lift_amount)
    block_ordering = jnp.where(admissible_blocks, extra_lift_amount[:, :, None] * overall_block_tally + precedence_rating, -1).reshape(MEMORY_GROUPS, overall_block_tally)
    picked = lax.top_k(block_ordering, K)[1]
    return picked.astype(jnp.int32)


def draw_queries(key, part):
    base = 2.0 * jax.random.normal(jax.random.fold_in(key, 21), (DRAFT, MEMORY_GROUPS * G, D), jnp.float32)
    return jnp.clip(base, -64.0, 64.0).reshape(DRAFT, MEMORY_GROUPS * G * D).astype(jnp.bfloat16)


def draw_key_cache(key, part):
    base = jax.random.normal(jax.random.fold_in(key, 31), (PPD * N_PAGE, PAGE, MEMORY_GROUPS * D), jnp.float32)
    return jnp.clip(base, -9.0, 9.0).astype(jnp.bfloat16)


def draw_value_cache(key, part):
    offsets = 1.5 * jax.random.normal(jax.random.fold_in(key, 41), (PPD * N_PAGE, 1, MEMORY_GROUPS * D), jnp.float32)
    noise = jax.random.normal(jax.random.fold_in(key, 42), (PPD * N_PAGE, PAGE, MEMORY_GROUPS * D), jnp.float32)
    return jnp.clip(noise + offsets, -16.0, 16.0).astype(jnp.bfloat16)


def bell_draw(rng, dims, scale, limit, kind=jnp.bfloat16):
    drawn = jax.random.normal(rng, dims, jnp.float32) * scale
    return jnp.minimum(jnp.maximum(drawn, -limit), limit).astype(kind)


def setup_inputs(seed: int = 0, part: int = 0) -> dict:
    seeds = jax.random.split(jax.random.key(seed), 7)
    part_splits = jax.random.split(jax.random.fold_in(seeds[6], part), 7)
    queries = draw_queries(jax.random.fold_in(jax.random.fold_in(seeds[6], part), 71), part)
    key_cache = draw_key_cache(jax.random.fold_in(jax.random.fold_in(seeds[6], part), 71), part)
    value_cache = draw_value_cache(jax.random.fold_in(jax.random.fold_in(seeds[6], part), 71), part)
    new_keys = bell_draw(part_splits[3], (DRAFT, MEMORY_GROUPS * D), 3.0, 16.0)
    new_values = bell_draw(part_splits[4], (DRAFT, MEMORY_GROUPS * D), 1.0, 6.0)
    chosen = draw_chosen(jax.random.fold_in(jax.random.fold_in(seeds[6], part), 71), part)
    return {"queries": queries, "key_cache": key_cache, "value_cache": value_cache, "new_keys": new_keys, "new_values": new_values, "chosen": chosen}


def reference(queries, key_cache, value_cache, new_keys, new_values, chosen):
    row_count = DRAFT * G
    scaling = D ** -0.5
    query_heads = queries.reshape(DRAFT, MEMORY_GROUPS, G, D).transpose(1, 0, 2, 3).reshape(MEMORY_GROUPS, row_count, D)
    key_fresh = new_keys.reshape(DRAFT, MEMORY_GROUPS, D).transpose(1, 0, 2)
    value_fresh = new_values.reshape(DRAFT, MEMORY_GROUPS, D).transpose(1, 0, 2)
    position = jnp.arange(row_count, dtype=jnp.int32) // G
    allowed = jnp.arange(DRAFT, dtype=jnp.int32)[None, :] <= position[:, None]

    def one_head(head_id):
        query_rows = query_heads[head_id]
        key_head = lax.dynamic_slice_in_dim(key_cache, head_id * D, D, 2)
        value_head = lax.dynamic_slice_in_dim(value_cache, head_id * D, D, 2)
        page_ids = chosen[head_id]
        key_rows = jnp.take(key_head, page_ids, axis=0).reshape(K * PAGE, D)
        value_rows = jnp.take(value_head, page_ids, axis=0).reshape(K * PAGE, D)
        cached = jnp.dot(query_rows, key_rows.T, preferred_element_type=jnp.float32) * scaling
        fresh_scores = jnp.dot(query_rows, key_fresh[head_id].T, preferred_element_type=jnp.float32) * scaling
        fresh_scores = jnp.where(allowed, fresh_scores, -jnp.inf)
        highest = jnp.maximum(jnp.max(cached, axis=1), jnp.max(fresh_scores, axis=1))
        weight_cached = jnp.exp(cached - highest[:, None]).astype(jnp.bfloat16)
        weight_fresh = jnp.where(allowed, jnp.exp(fresh_scores - highest[:, None]), 0.0).astype(jnp.bfloat16)
        totals = jnp.sum(weight_cached.astype(jnp.float32), axis=1) + jnp.sum(weight_fresh.astype(jnp.float32), axis=1)
        weighted = jnp.dot(weight_cached, value_rows, preferred_element_type=jnp.float32)
        weighted = weighted + jnp.dot(weight_fresh, value_fresh[head_id], preferred_element_type=jnp.float32)
        return (weighted / totals[:, None]).astype(jnp.bfloat16)

    attended = lax.map(one_head, jnp.arange(MEMORY_GROUPS, dtype=jnp.int32))
    return attended.reshape(MEMORY_GROUPS, DRAFT, G, D).transpose(1, 0, 2, 3).reshape(DRAFT, MEMORY_GROUPS * G * D)
```

```python
import jax
import jax.numpy as jnp
from jax import lax
from jax.experimental import pallas as pl
from jax.experimental.pallas import tpu as pltpu
from jax.sharding import Mesh
from jax.sharding import PartitionSpec as P

GRP_PAGE = ("grp", "page_0", "page_1", "page_2")
PAGE = GRP_PAGE[1:]
FLOOR = -1e30
F32 = jnp.float32
BF16 = jnp.bfloat16
MESH = pl.DeviceIdType.MESH


def dot_nt(a, b):
    return lax.dot_general(a, b, (((1,), (1,)), ((), ())), preferred_element_type=F32)


def dot_nn(a, b):
    return lax.dot_general(a, b, (((1,), (0,)), ((), ())), preferred_element_type=F32)


def rows_of(ref, count):
    return jnp.concatenate([ref[i] for i in range(count)], axis=0)


def flip(x):
    n = x.shape[0]
    if n < 128:
        x = jnp.concatenate([x, jnp.zeros((128 - n, 128), x.dtype)], axis=0)
    return jnp.transpose(x)


def merge_weights(lse):
    top = jnp.max(lse, axis=0, keepdims=True)
    w = jnp.exp(lse - top)
    total = jnp.sum(w, axis=0, keepdims=True)
    return w / total, top + jnp.log(total)


def far_first(n, ring):
    def key(d):
        return -min(d // ring, (n - d) // ring)

    return sorted(range(1, n), key=key)


def make_kernel(nz, nx, nc, heads, tokens, page_tokens, drafts, groups, scaling):
    na = nx * nc * 2
    nb = nz // 2
    pages = tokens // page_tokens
    block_rows = heads * groups * drafts // na
    per_head = na // heads
    width = block_rows // drafts * 128

    def kernel(
        q_ref, ids_ref, nk_ref, nv_ref, k_hbm, v_hbm, out_ref,
        ks, vs, s_ref, idbs, idbr, idas, idar,
        o1s, l1s, o1r, l1r, o2s, l2s, o2r, l2r, fs, fr, msc, ex,
        k_sem, v_sem, b_send, b_recv, a_send, a_recv,
        o1_send, o1_recv, l1_send, l1_recv,
        o2_send, o2_recv, l2_send, l2_recv, f_send, f_recv,
    ):
        z = lax.axis_index("page_0")
        x = lax.axis_index("page_1")
        c = lax.axis_index("page_2")
        zlow = lax.rem(z, 2)
        b = lax.div(z, 2)
        a = (x * nc + c) * 2 + zlow

        def a_dev(d):
            t = lax.rem(a + d, na)
            u = lax.div(t, 2)
            return t, {
                "page_0": b * 2 + lax.rem(t, 2),
                "page_1": lax.div(u, nc),
                "page_2": lax.rem(u, nc),
            }

        def b_dev(d):
            t = lax.rem(b + d, nb)
            return t, {"page_0": t * 2 + zlow, "page_1": x, "page_2": c}

        order_a = far_first(na, nc * 2)
        order_b = far_first(nb, 1)

        def copy(src, dst, ss, rs, dev):
            return pltpu.make_async_remote_copy(
                src_ref=src, dst_ref=dst, send_sem=ss, recv_sem=rs,
                device_id=dev, device_id_type=MESH,
            )

        def send(group, order, src, dst, me, ss, rs):
            started = []
            for d in order:
                t, dev = group(d)
                r = copy(src(t), dst.at[me], ss.at[d], rs.at[me], dev)
                r.start()
                started.append(r)
            return started

        def wait_all(group, order, src, dst, n, ss, rs):
            for d in order[::-1]:
                t, dev = group(n - d)
                copy(src(t), dst.at[t], ss.at[n - d], rs.at[t], dev).wait_recv()

        barrier = pltpu.get_barrier_semaphore()
        for d in order_b:
            pl.semaphore_signal(barrier, inc=1, device_id=b_dev(d)[1], device_id_type=MESH)
        for d in order_a:
            pl.semaphore_signal(barrier, inc=1, device_id=a_dev(d)[1], device_id_type=MESH)

        def load(src, dst, sem, h):
            return pltpu.make_async_copy(src.at[:, pl.ds(h * 128, 128)], dst.at[h], sem.at[h])

        for h in range(heads):
            load(k_hbm, ks, k_sem, h).start()
        for h in range(heads):
            load(v_hbm, vs, v_sem, h).start()

        lane = lax.broadcasted_iota(jnp.int32, (1, 128), 1)
        slot = 128 // nb
        idbs[...] = jnp.where(lax.div(lane, slot) == b, ids_ref[...], 0)
        idbr[b] = idbs[...]

        def scores(h):
            load(k_hbm, ks, k_sem, h).wait()
            base = h * groups * 128
            q = jnp.concatenate(
                [q_ref[:, base + g * 128 : base + (g + 1) * 128] for g in range(groups)], axis=0
            )
            s_ref[h] = dot_nt(q, ks[h]) * scaling

        half = heads // 2
        for h in range(half):
            scores(h)

        cols = pl.multiple_of(a * width, width)
        head_cols = pl.multiple_of(lax.div(a, per_head) * 128, 128)
        q_own = q_ref[:, pl.ds(cols, width)]
        q_own = jnp.concatenate(
            [q_own[:, i * 128 : (i + 1) * 128] for i in range(width // 128)], axis=0
        )
        pad = jnp.zeros((128 - drafts, 128), BF16)
        kf = jnp.concatenate([nk_ref[:, pl.ds(head_cols, 128)], pad], axis=0)
        vf = jnp.concatenate([nv_ref[:, pl.ds(head_cols, 128)], pad], axis=0)
        sf = dot_nt(q_own, kf) * scaling
        pos = lax.rem(lax.broadcasted_iota(jnp.int32, sf.shape, 0), drafts)
        ok = lax.broadcasted_iota(jnp.int32, sf.shape, 1) <= pos
        sf = jnp.where(ok, sf, FLOOR)
        mf = jnp.max(sf, axis=1, keepdims=True)
        pf = jnp.where(ok, jnp.exp(sf - mf), 0.0).astype(BF16)
        tf = jnp.sum(pf.astype(F32), axis=1, keepdims=True)
        of = dot_nn(pf, vf) / tf
        lf = flip(jnp.broadcast_to(mf + jnp.log(tf), (block_rows, 128)))[0:1]

        key_page = lax.div(lax.broadcasted_iota(jnp.int32, (128, tokens), 1), page_tokens)
        row_page = lax.broadcasted_iota(jnp.int32, (128, tokens), 0)
        ex[...] = (key_page == row_page).astype(F32).astype(BF16)

        pl.semaphore_wait(barrier, na - 1 + nb - 1)
        sent = send(b_dev, order_b, lambda t: idbs, idbr, b, b_send, b_recv)
        for h in range(half, heads):
            scores(h)
        wait_all(b_dev, order_b, lambda t: idbs, idbr, nb, b_send, b_recv)
        joined = idbr[0]
        for i in range(1, nb):
            joined = joined + idbr[i]
        idas[...] = joined
        idar[a] = joined
        sent += send(a_dev, order_a, lambda t: idas, idar, a, a_send, a_recv)
        for h in range(heads):
            load(v_hbm, vs, v_sem, h).wait()
        wait_all(a_dev, order_a, lambda t: idas, idar, na, a_send, a_recv)

        local = rows_of(idar, na) - ((z * nx + x) * nc + c) * pages
        counts = [
            jnp.sum((local == p).astype(F32), axis=0, keepdims=True) for p in range(pages)
        ]
        counts.append(jnp.zeros((128 - pages, 128), F32))
        counts = jnp.concatenate(counts, axis=0).astype(BF16)
        lane_head = lax.div(lax.rem(lax.broadcasted_iota(jnp.int32, (heads, 128), 1), slot), slot // heads)
        pick = (lane_head == lax.broadcasted_iota(jnp.int32, (heads, 128), 0)).astype(F32).astype(BF16)
        picked = dot_nt(pick, counts).astype(BF16)
        usable = dot_nn(picked, ex[...])

        lanes = lax.broadcasted_iota(jnp.int32, (block_rows, 128), 1)
        stats = jnp.zeros((block_rows, 128), F32)
        for h in range(heads):
            s = jnp.where(usable[h : h + 1] > 0.5, s_ref[h], FLOOR)
            top = jnp.max(s, axis=1, keepdims=True)
            offset = jnp.where(top > 0.5 * FLOOR, top, 0.0)
            p = jnp.exp(s - offset).astype(BF16)
            total = jnp.sum(p.astype(F32), axis=1, keepdims=True)
            safe = jnp.maximum(total, 0.5)
            o = dot_nn(p, vs[h]) / safe
            lse = jnp.where(total > 0.0, offset + jnp.log(safe), FLOOR)
            for i in range(per_head):
                part = slice(i * block_rows, (i + 1) * block_rows)
                o1s[h * per_head + i] = o[part].astype(BF16)
                stats = jnp.where(lanes == h * per_head + i, lse[part], stats)
        stats = flip(stats)
        for i in range(na):
            l1s[i] = stats[i : i + 1]
        l1r[a] = l1s[a]
        o1r[a] = o1s[a]
        sent += send(a_dev, order_a, lambda t: l1s.at[t], l1r, a, l1_send, l1_recv)
        sent += send(a_dev, order_a, lambda t: o1s.at[t], o1r, a, o1_send, o1_recv)
        wait_all(a_dev, order_a, lambda t: l1s.at[t], l1r, na, l1_send, l1_recv)
        w, lse = merge_weights(rows_of(l1r, na))
        w = flip(w)[0:block_rows]
        l2s[...] = lse
        l2r[b] = lse
        sent += send(b_dev, order_b, lambda t: l2s, l2r, b, l2_send, l2_recv)
        wait_all(a_dev, order_a, lambda t: o1s.at[t], o1r, na, o1_send, o1_recv)
        o = w[:, 0:1] * o1r[0].astype(F32)
        for i in range(1, na):
            o = o + w[:, i : i + 1] * o1r[i].astype(F32)
        o = o.astype(BF16)
        o2s[...] = o
        o2r[b] = o
        sent += send(b_dev, order_b, lambda t: o2s, o2r, b, o2_send, o2_recv)
        wait_all(b_dev, order_b, lambda t: l2s, l2r, nb, l2_send, l2_recv)
        w, _ = merge_weights(jnp.concatenate([lf, rows_of(l2r, nb)], axis=0))
        w = flip(w)[0:block_rows]
        o = w[:, 0:1] * of
        wait_all(b_dev, order_b, lambda t: o2s, o2r, nb, o2_send, o2_recv)
        for i in range(nb):
            o = o + w[:, i + 1 : i + 2] * o2r[i].astype(F32)
        o = o.astype(BF16)
        block = jnp.concatenate(
            [o[i * drafts : (i + 1) * drafts] for i in range(width // 128)], axis=1
        )
        fs[...] = block
        fr[a] = block
        sent += send(a_dev, order_a, lambda t: fs, fr, a, f_send, f_recv)
        wait_all(a_dev, order_a, lambda t: fs, fr, na, f_send, f_recv)
        for i in range(na):
            out_ref[:, i * width : (i + 1) * width] = fr[i]
        for r in sent:
            r.wait_send()

    dma = pltpu.SemaphoreType.DMA
    span = heads * 128
    rows = heads * groups * drafts // heads
    scratch = [
        pltpu.VMEM((heads, tokens, 128), BF16),
        pltpu.VMEM((heads, tokens, 128), BF16),
        pltpu.VMEM((heads, rows, tokens), F32),
        pltpu.VMEM((1, 128), jnp.int32),
        pltpu.VMEM((nb, 1, 128), jnp.int32),
        pltpu.VMEM((1, 128), jnp.int32),
        pltpu.VMEM((na, 1, 128), jnp.int32),
        pltpu.VMEM((na, block_rows, 128), BF16),
        pltpu.VMEM((na, 1, 128), F32),
        pltpu.VMEM((na, block_rows, 128), BF16),
        pltpu.VMEM((na, 1, 128), F32),
        pltpu.VMEM((block_rows, 128), BF16),
        pltpu.VMEM((1, 128), F32),
        pltpu.VMEM((nb, block_rows, 128), BF16),
        pltpu.VMEM((nb, 1, 128), F32),
        pltpu.VMEM((drafts, width), BF16),
        pltpu.VMEM((na, drafts, width), BF16),
        pltpu.VMEM((block_rows, 128), F32),
        pltpu.VMEM((128, tokens), BF16),
        dma((heads,)), dma((heads,)),
        dma((nb,)), dma((nb,)), dma((na,)), dma((na,)),
        dma((na,)), dma((na,)), dma((na,)), dma((na,)),
        dma((nb,)), dma((nb,)), dma((nb,)), dma((nb,)), dma((na,)), dma((na,)),
    ]
    vmem = pl.BlockSpec(memory_space=pltpu.VMEM)
    anyspace = pl.BlockSpec(memory_space=pl.ANY)
    return pl.pallas_call(
        kernel,
        out_shape=jax.ShapeDtypeStruct((drafts, heads * groups * 128), BF16),
        in_specs=[vmem, vmem, vmem, vmem, anyspace, anyspace],
        out_specs=vmem,
        scratch_shapes=scratch,
        compiler_params=pltpu.CompilerParams(
            collective_id=0, has_side_effects=True, vmem_limit_bytes=48 * 1024 * 1024
        ),
    )


def solution(mesh):
    nz, nx, nc = 16, 4, 2
    torus = Mesh(
        mesh.devices.reshape(mesh.shape["grp"], nz, nx, nc), ("grp", "page_0", "page_1", "page_2")
    )

    def on_device(queries, key_cache, value_cache, new_keys, new_values, chosen):
        pages, page_tokens, span = key_cache.shape
        heads = chosen.shape[0]
        drafts = queries.shape[0]
        groups = queries.shape[1] // span
        call = make_kernel(
            nz, nx, nc, heads, pages * page_tokens, page_tokens, drafts, groups,
            (span // heads) ** (-0.5),
        )
        ids = jnp.tile(chosen.reshape(1, -1), (1, 128 // chosen.size))
        return call(
            queries, ids, new_keys, new_values,
            key_cache.reshape(-1, span), value_cache.reshape(-1, span),
        )

    in_specs = (
        P("grp", None),
        P(GRP_PAGE, None, None),
        P(GRP_PAGE, None, None),
        P("grp", None),
        P("grp", None),
        P("grp", PAGE),
    )
    return jax.shard_map(
        on_device, mesh=torus, in_specs=in_specs, out_specs=P("grp", None), check_vma=False
    )
```

```python
import jax
import jax.numpy as jnp
from jax import lax
from jax.experimental import pallas as pl
from jax.experimental.pallas import tpu as pltpu
from jax.sharding import Mesh
from jax.sharding import PartitionSpec as P

GRP_PAGE = ("grp", "page_0", "page_1", "page_2")
PAGE = GRP_PAGE[1:]
FLOOR = -1e30
F32 = jnp.float32
BF16 = jnp.bfloat16
MESH = pl.DeviceIdType.MESH


def dot_nt(a, b):
    return lax.dot_general(a, b, (((1,), (1,)), ((), ())), preferred_element_type=F32)


def dot_nn(a, b):
    return lax.dot_general(a, b, (((1,), (0,)), ((), ())), preferred_element_type=F32)


def rows_of(ref, count):
    return jnp.concatenate([ref[i] for i in range(count)], axis=0)


def flip(x):
    n = x.shape[0]
    if n < 128:
        x = jnp.concatenate([x, jnp.zeros((128 - n, 128), x.dtype)], axis=0)
    return jnp.transpose(x)


def merge_weights(lse):
    top = jnp.max(lse, axis=0, keepdims=True)
    w = jnp.exp(lse - top)
    total = jnp.sum(w, axis=0, keepdims=True)
    return w / total, top + jnp.log(total)


def far_first(n, ring):
    def key(d):
        return -min(d // ring, (n - d) // ring)

    return sorted(range(1, n), key=key)


def make_kernel(nz, nx, nc, heads, tokens, page_tokens, drafts, groups, scaling):
    na = nx * nc * 2
    nb = nz // 2
    pages = tokens // page_tokens
    block_rows = heads * groups * drafts // na
    per_head = na // heads
    width = block_rows // drafts * 128

    def kernel(
        q_hbm, ids_hbm, nk_hbm, nv_hbm, k_hbm, v_hbm, out_ref,
        q_ref, ids_ref, nk_ref, nv_ref, small_sem, ks, vs, s_ref, idbs, idbr, idas, idar,
        o1s, l1s, o1r, l1r, o2s, l2s, o2r, l2r, fs, fr, ex,
        k_sem, v_sem, b_send, b_recv, a_send, a_recv,
        o1_send, o1_recv, l1_send, l1_recv,
        o2_send, o2_recv, l2_send, l2_recv, f_send, f_recv,
    ):
        z = lax.axis_index("page_0")
        x = lax.axis_index("page_1")
        c = lax.axis_index("page_2")
        zlow = lax.rem(z, 2)
        b = lax.div(z, 2)
        a = (x * nc + c) * 2 + zlow

        def a_dev(d):
            t = lax.rem(a + d, na)
            u = lax.div(t, 2)
            return t, {
                "page_0": b * 2 + lax.rem(t, 2),
                "page_1": lax.div(u, nc),
                "page_2": lax.rem(u, nc),
            }

        def b_dev(d):
            t = lax.rem(b + d, nb)
            return t, {"page_0": t * 2 + zlow, "page_1": x, "page_2": c}

        order_a = far_first(na, nc * 2)
        order_b = far_first(nb, 1)

        def copy(src, dst, ss, rs, dev):
            return pltpu.make_async_remote_copy(
                src_ref=src, dst_ref=dst, send_sem=ss, recv_sem=rs,
                device_id=dev, device_id_type=MESH,
            )

        def send(group, order, src, dst, me, ss, rs):
            started = []
            for d in order:
                t, dev = group(d)
                r = copy(src(t), dst.at[me], ss.at[d], rs.at[me], dev)
                r.start()
                started.append(r)
            return started

        def wait_all(group, order, src, dst, n, ss, rs):
            for d in order[::-1]:
                t, dev = group(n - d)
                copy(src(t), dst.at[t], ss.at[n - d], rs.at[t], dev).wait_recv()

        small = [
            pltpu.make_async_copy(src, dst, small_sem.at[i])
            for i, (src, dst) in enumerate(
                [(ids_hbm, ids_ref), (q_hbm, q_ref), (nk_hbm, nk_ref), (nv_hbm, nv_ref)]
            )
        ]
        small[0].start()
        barrier = pltpu.get_barrier_semaphore()
        for d in order_b:
            pl.semaphore_signal(barrier, inc=1, device_id=b_dev(d)[1], device_id_type=MESH)
        for d in order_a:
            pl.semaphore_signal(barrier, inc=1, device_id=a_dev(d)[1], device_id_type=MESH)

        def load(src, dst, sem, h):
            return pltpu.make_async_copy(src.at[:, pl.ds(h * 128, 128)], dst.at[h], sem.at[h])

        for r in small[1:]:
            r.start()
        for h in range(heads):
            load(k_hbm, ks, k_sem, h).start()
        for h in range(heads):
            load(v_hbm, vs, v_sem, h).start()

        lane = lax.broadcasted_iota(jnp.int32, (1, 128), 1)
        slot = 128 // nb
        small[0].wait()
        ids = ids_ref[...]
        ids = jnp.concatenate([ids[j : j + 1] for j in range(ids.shape[0])] * nb, axis=1)
        idbs[...] = jnp.where(lax.div(lane, slot) == b, ids, 0)
        idbr[b] = idbs[...]

        def scores(h):
            load(k_hbm, ks, k_sem, h).wait()
            base = h * groups * 128
            q = jnp.concatenate(
                [q_ref[:, base + g * 128 : base + (g + 1) * 128] for g in range(groups)], axis=0
            )
            s_ref[h] = dot_nt(q, ks[h]) * scaling

        pl.semaphore_wait(barrier, na - 1 + nb - 1)
        sent = send(b_dev, order_b, lambda t: idbs, idbr, b, b_send, b_recv)
        for r in small[1:]:
            r.wait()
        for h in range(heads):
            scores(h)

        cols = pl.multiple_of(a * width, width)
        head_cols = pl.multiple_of(lax.div(a, per_head) * 128, 128)
        q_own = q_ref[:, pl.ds(cols, width)]
        q_own = jnp.concatenate(
            [q_own[:, i * 128 : (i + 1) * 128] for i in range(width // 128)], axis=0
        )
        pad = jnp.zeros((128 - drafts, 128), BF16)
        kf = jnp.concatenate([nk_ref[:, pl.ds(head_cols, 128)], pad], axis=0)
        vf = jnp.concatenate([nv_ref[:, pl.ds(head_cols, 128)], pad], axis=0)
        sf = dot_nt(q_own, kf) * scaling
        pos = lax.rem(lax.broadcasted_iota(jnp.int32, sf.shape, 0), drafts)
        ok = lax.broadcasted_iota(jnp.int32, sf.shape, 1) <= pos
        sf = jnp.where(ok, sf, FLOOR)
        mf = jnp.max(sf, axis=1, keepdims=True)
        pf = jnp.where(ok, jnp.exp(sf - mf), 0.0).astype(BF16)
        tf = jnp.sum(pf.astype(F32), axis=1, keepdims=True)
        of = dot_nn(pf, vf) / tf
        lf = flip(jnp.broadcast_to(mf + jnp.log(tf), (block_rows, 128)))[0:1]

        key_page = lax.div(lax.broadcasted_iota(jnp.int32, (128, tokens), 1), page_tokens)
        row_page = lax.broadcasted_iota(jnp.int32, (128, tokens), 0)
        ex[...] = (key_page == row_page).astype(F32).astype(BF16)

        wait_all(b_dev, order_b, lambda t: idbs, idbr, nb, b_send, b_recv)
        joined = idbr[0]
        for i in range(1, nb):
            joined = joined + idbr[i]
        idas[...] = joined
        idar[a] = joined
        sent += send(a_dev, order_a, lambda t: idas, idar, a, a_send, a_recv)
        for h in range(heads):
            load(v_hbm, vs, v_sem, h).wait()
        wait_all(a_dev, order_a, lambda t: idas, idar, na, a_send, a_recv)

        local = rows_of(idar, na) - ((z * nx + x) * nc + c) * pages
        counts = [
            jnp.sum((local == p).astype(F32), axis=0, keepdims=True) for p in range(pages)
        ]
        counts.append(jnp.zeros((128 - pages, 128), F32))
        counts = jnp.concatenate(counts, axis=0).astype(BF16)
        lane_head = lax.rem(lax.broadcasted_iota(jnp.int32, (heads, 128), 1), heads)
        pick = (lane_head == lax.broadcasted_iota(jnp.int32, (heads, 128), 0)).astype(F32).astype(BF16)
        picked = dot_nt(pick, counts).astype(BF16)
        usable = dot_nn(picked, ex[...])

        lanes = lax.broadcasted_iota(jnp.int32, (block_rows, 128), 1)
        stats = jnp.zeros((block_rows, 128), F32)
        for h in range(heads):
            s = jnp.where(usable[h : h + 1] > 0.5, s_ref[h], FLOOR)
            top = jnp.max(s, axis=1, keepdims=True)
            offset = jnp.where(top > 0.5 * FLOOR, top, 0.0)
            p = jnp.exp(s - offset).astype(BF16)
            total = jnp.sum(p.astype(F32), axis=1, keepdims=True)
            safe = jnp.maximum(total, 0.5)
            o = dot_nn(p, vs[h]) / safe
            lse = jnp.where(total > 0.0, offset + jnp.log(safe), FLOOR)
            for i in range(per_head):
                part = slice(i * block_rows, (i + 1) * block_rows)
                o1s[h * per_head + i] = o[part].astype(BF16)
                stats = jnp.where(lanes == h * per_head + i, lse[part], stats)
        stats = flip(stats)
        for i in range(na):
            l1s[i] = stats[i : i + 1]
        l1r[a] = l1s[a]
        o1r[a] = o1s[a]
        sent += send(a_dev, order_a, lambda t: l1s.at[t], l1r, a, l1_send, l1_recv)
        sent += send(a_dev, order_a, lambda t: o1s.at[t], o1r, a, o1_send, o1_recv)
        wait_all(a_dev, order_a, lambda t: l1s.at[t], l1r, na, l1_send, l1_recv)
        w, lse = merge_weights(rows_of(l1r, na))
        w = flip(w)[0:block_rows]
        l2s[...] = lse
        l2r[b] = lse
        sent += send(b_dev, order_b, lambda t: l2s, l2r, b, l2_send, l2_recv)
        wait_all(a_dev, order_a, lambda t: o1s.at[t], o1r, na, o1_send, o1_recv)
        o = w[:, 0:1] * o1r[0].astype(F32)
        for i in range(1, na):
            o = o + w[:, i : i + 1] * o1r[i].astype(F32)
        o = o.astype(BF16)
        o2s[...] = o
        o2r[b] = o
        sent += send(b_dev, order_b, lambda t: o2s, o2r, b, o2_send, o2_recv)
        wait_all(b_dev, order_b, lambda t: l2s, l2r, nb, l2_send, l2_recv)
        w, _ = merge_weights(jnp.concatenate([lf, rows_of(l2r, nb)], axis=0))
        w = flip(w)[0:block_rows]
        o = w[:, 0:1] * of
        wait_all(b_dev, order_b, lambda t: o2s, o2r, nb, o2_send, o2_recv)
        for i in range(nb):
            o = o + w[:, i + 1 : i + 2] * o2r[i].astype(F32)
        o = o.astype(BF16)
        block = jnp.concatenate(
            [o[i * drafts : (i + 1) * drafts] for i in range(width // 128)], axis=1
        )
        fs[...] = block
        fr[a] = block
        sent += send(a_dev, order_a, lambda t: fs, fr, a, f_send, f_recv)
        wait_all(a_dev, order_a, lambda t: fs, fr, na, f_send, f_recv)
        for i in range(na):
            out_ref[:, i * width : (i + 1) * width] = fr[i]
        for r in sent:
            r.wait_send()

    dma = pltpu.SemaphoreType.DMA
    span = heads * 128
    rows = heads * groups * drafts // heads
    scratch = [
        pltpu.VMEM((drafts, heads * groups * 128), BF16),
        pltpu.VMEM((128 // nb // heads, heads), jnp.int32),
        pltpu.VMEM((drafts, span), BF16),
        pltpu.VMEM((drafts, span), BF16),
        dma((4,)),
        pltpu.VMEM((heads, tokens, 128), BF16),
        pltpu.VMEM((heads, tokens, 128), BF16),
        pltpu.VMEM((heads, rows, tokens), F32),
        pltpu.VMEM((1, 128), jnp.int32),
        pltpu.VMEM((nb, 1, 128), jnp.int32),
        pltpu.VMEM((1, 128), jnp.int32),
        pltpu.VMEM((na, 1, 128), jnp.int32),
        pltpu.VMEM((na, block_rows, 128), BF16),
        pltpu.VMEM((na, 1, 128), F32),
        pltpu.VMEM((na, block_rows, 128), BF16),
        pltpu.VMEM((na, 1, 128), F32),
        pltpu.VMEM((block_rows, 128), BF16),
        pltpu.VMEM((1, 128), F32),
        pltpu.VMEM((nb, block_rows, 128), BF16),
        pltpu.VMEM((nb, 1, 128), F32),
        pltpu.VMEM((drafts, width), BF16),
        pltpu.VMEM((na, drafts, width), BF16),
        pltpu.VMEM((128, tokens), BF16),
        dma((heads,)), dma((heads,)),
        dma((nb,)), dma((nb,)), dma((na,)), dma((na,)),
        dma((na,)), dma((na,)), dma((na,)), dma((na,)),
        dma((nb,)), dma((nb,)), dma((nb,)), dma((nb,)), dma((na,)), dma((na,)),
    ]
    vmem = pl.BlockSpec(memory_space=pltpu.VMEM)
    hbm = pl.BlockSpec(memory_space=pltpu.HBM)
    return pl.pallas_call(
        kernel,
        out_shape=jax.ShapeDtypeStruct((drafts, heads * groups * 128), BF16),
        in_specs=[hbm] * 6,
        out_specs=vmem,
        scratch_shapes=scratch,
        compiler_params=pltpu.CompilerParams(
            collective_id=0, has_side_effects=True, vmem_limit_bytes=60 * 1024 * 1024
        ),
    )


def solution(mesh):
    nz, nx, nc = 16, 4, 2
    torus = Mesh(
        mesh.devices.reshape(mesh.shape["grp"], nz, nx, nc), ("grp", "page_0", "page_1", "page_2")
    )

    def on_device(queries, key_cache, value_cache, new_keys, new_values, chosen):
        pages, page_tokens, span = key_cache.shape
        heads = chosen.shape[0]
        drafts = queries.shape[0]
        groups = queries.shape[1] // span
        call = make_kernel(
            nz, nx, nc, heads, pages * page_tokens, page_tokens, drafts, groups,
            (span // heads) ** (-0.5),
        )
        return call(
            queries, chosen.T, new_keys, new_values,
            key_cache.reshape(-1, span), value_cache.reshape(-1, span),
        )

    in_specs = (
        P("grp", None),
        P(GRP_PAGE, None, None),
        P(GRP_PAGE, None, None),
        P("grp", None),
        P("grp", None),
        P("grp", PAGE),
    )
    return jax.shard_map(
        on_device, mesh=torus, in_specs=in_specs, out_specs=P("grp", None), check_vma=False
    )
```

```python
import jax
import jax.numpy as jnp
from jax import lax
from jax.experimental import pallas as pl
from jax.experimental.pallas import tpu as pltpu
from jax.sharding import Mesh
from jax.sharding import PartitionSpec as P

GRP_PAGE = ("grp", "page_0", "page_1", "page_2")
PAGE = GRP_PAGE[1:]
FLOOR = -1e30
F32 = jnp.float32
BF16 = jnp.bfloat16
MESH = pl.DeviceIdType.MESH


def dot_nt(a, b):
    return lax.dot_general(a, b, (((1,), (1,)), ((), ())), preferred_element_type=F32)


def dot_nn(a, b):
    return lax.dot_general(a, b, (((1,), (0,)), ((), ())), preferred_element_type=F32)


def rows_of(ref, count):
    return jnp.concatenate([ref[i] for i in range(count)], axis=0)


def flip(x):
    n = x.shape[0]
    if n < 128:
        x = jnp.concatenate([x, jnp.zeros((128 - n, 128), x.dtype)], axis=0)
    return jnp.transpose(x)


def merge_weights(lse):
    top = jnp.max(lse, axis=0, keepdims=True)
    w = jnp.exp(lse - top)
    total = jnp.sum(w, axis=0, keepdims=True)
    return w / total, top + jnp.log(total)


def far_first(n, ring):
    def key(d):
        return -min(d // ring, (n - d) // ring)

    return sorted(range(1, n), key=key)


def make_kernel(nz, nx, nc, heads, tokens, page_tokens, drafts, groups, scaling):
    na = nx * nc * 2
    nb = nz // 2
    pages = tokens // page_tokens
    block_rows = heads * groups * drafts // na
    per_head = na // heads
    width = block_rows // drafts * 128

    def kernel(
        q_hbm, ids_hbm, nk_hbm, nv_hbm, k_hbm, v_hbm, out_ref,
        q_ref, ids_ref, nk_ref, nv_ref, small_sem, ks, vs, s_ref, idbs, idbr, idas, idar,
        o1s, l1s, o1r, l1r, o2s, l2s, o2r, l2r, fs, fr, ex, us,
        k_sem, v_sem, b_send, b_recv, a_send, a_recv,
        o1_send, o1_recv, l1_send, l1_recv,
        o2_send, o2_recv, l2_send, l2_recv, f_send, f_recv,
    ):
        z = lax.axis_index("page_0")
        x = lax.axis_index("page_1")
        c = lax.axis_index("page_2")
        zlow = lax.rem(z, 2)
        b = lax.div(z, 2)
        a = (x * nc + c) * 2 + zlow

        def a_dev(d):
            t = lax.rem(a + d, na)
            u = lax.div(t, 2)
            return t, {
                "page_0": b * 2 + lax.rem(t, 2),
                "page_1": lax.div(u, nc),
                "page_2": lax.rem(u, nc),
            }

        def b_dev(d):
            t = lax.rem(b + d, nb)
            return t, {"page_0": t * 2 + zlow, "page_1": x, "page_2": c}

        order_a = far_first(na, nc * 2)
        order_b = far_first(nb, 1)

        def copy(src, dst, ss, rs, dev):
            return pltpu.make_async_remote_copy(
                src_ref=src, dst_ref=dst, send_sem=ss, recv_sem=rs,
                device_id=dev, device_id_type=MESH,
            )

        def send(group, order, src, dst, me, ss, rs):
            started = []
            for d in order:
                t, dev = group(d)
                r = copy(src(t), dst.at[me], ss.at[d], rs.at[me], dev)
                r.start()
                started.append(r)
            return started

        def wait_all(group, order, src, dst, n, ss, rs):
            for d in order[::-1]:
                t, dev = group(n - d)
                copy(src(t), dst.at[t], ss.at[n - d], rs.at[t], dev).wait_recv()

        small = [
            pltpu.make_async_copy(src, dst, small_sem.at[i])
            for i, (src, dst) in enumerate(
                [(ids_hbm, ids_ref), (q_hbm, q_ref), (nk_hbm, nk_ref), (nv_hbm, nv_ref)]
            )
        ]
        small[0].start()
        def send_pairs(src, dst, ss, rs):
            for t in range(nb):
                d = lax.rem(t - b + nb, nb)

                @pl.when(d != 0)
                def _():
                    copy(src, dst.at[b], ss.at[d], rs.at[b], b_dev(d)[1]).start()

            return [copy(src, dst.at[b], ss.at[d], rs.at[b], b_dev(d)[1]) for d in order_b]

        barrier = pltpu.get_barrier_semaphore()
        for d in order_b:
            pl.semaphore_signal(barrier, inc=1, device_id=b_dev(d)[1], device_id_type=MESH)
        for d in order_a:
            pl.semaphore_signal(barrier, inc=1, device_id=a_dev(d)[1], device_id_type=MESH)

        def load(src, dst, sem, h):
            return pltpu.make_async_copy(src.at[:, pl.ds(h * 128, 128)], dst.at[h], sem.at[h])

        for r in small[1:]:
            r.start()
        for h in range(heads):
            load(k_hbm, ks, k_sem, h).start()
        for h in range(heads):
            load(v_hbm, vs, v_sem, h).start()

        lane = lax.broadcasted_iota(jnp.int32, (1, 128), 1)
        slot = 128 // nb
        small[0].wait()
        ids = ids_ref[...]
        ids = jnp.concatenate([ids[j : j + 1] for j in range(ids.shape[0])] * nb, axis=1)
        idbs[...] = jnp.where(lax.div(lane, slot) == b, ids, 0)
        idbr[b] = idbs[...]

        def scores(h):
            load(k_hbm, ks, k_sem, h).wait()
            base = h * groups * 128
            q = jnp.concatenate(
                [q_ref[:, base + g * 128 : base + (g + 1) * 128] for g in range(groups)], axis=0
            )
            s_ref[h] = dot_nt(q, ks[h]) * scaling

        pl.semaphore_wait(barrier, na - 1 + nb - 1)
        sent = send(b_dev, order_b, lambda t: idbs, idbr, b, b_send, b_recv)
        for r in small[1:]:
            r.wait()
        for h in range(heads):
            scores(h)

        cols = pl.multiple_of(a * width, width)
        head_cols = pl.multiple_of(lax.div(a, per_head) * 128, 128)
        q_own = q_ref[:, pl.ds(cols, width)]
        q_own = jnp.concatenate(
            [q_own[:, i * 128 : (i + 1) * 128] for i in range(width // 128)], axis=0
        )
        pad = jnp.zeros((128 - drafts, 128), BF16)
        kf = jnp.concatenate([nk_ref[:, pl.ds(head_cols, 128)], pad], axis=0)
        vf = jnp.concatenate([nv_ref[:, pl.ds(head_cols, 128)], pad], axis=0)
        sf = dot_nt(q_own, kf) * scaling
        pos = lax.rem(lax.broadcasted_iota(jnp.int32, sf.shape, 0), drafts)
        ok = lax.broadcasted_iota(jnp.int32, sf.shape, 1) <= pos
        sf = jnp.where(ok, sf, FLOOR)
        mf = jnp.max(sf, axis=1, keepdims=True)
        pf = jnp.where(ok, jnp.exp(sf - mf), 0.0).astype(BF16)
        tf = jnp.sum(pf.astype(F32), axis=1, keepdims=True)
        of = dot_nn(pf, vf) / tf
        lf = flip(jnp.broadcast_to(mf + jnp.log(tf), (block_rows, 128)))[0:1]

        key_page = lax.div(lax.broadcasted_iota(jnp.int32, (128, tokens), 1), page_tokens)
        row_page = lax.broadcasted_iota(jnp.int32, (128, tokens), 0)
        ex[...] = (key_page == row_page).astype(F32).astype(BF16)

        wait_all(b_dev, order_b, lambda t: idbs, idbr, nb, b_send, b_recv)
        joined = idbr[0]
        for i in range(1, nb):
            joined = joined + idbr[i]
        idas[...] = joined
        idar[a] = joined
        sent += send(a_dev, order_a, lambda t: idas, idar, a, a_send, a_recv)
        for h in range(heads):
            load(v_hbm, vs, v_sem, h).wait()
        wait_all(a_dev, order_a, lambda t: idas, idar, na, a_send, a_recv)

        local = rows_of(idar, na) - ((z * nx + x) * nc + c) * pages
        counts = [
            jnp.sum((local == p).astype(F32), axis=0, keepdims=True) for p in range(pages)
        ]
        counts.append(jnp.zeros((128 - pages, 128), F32))
        counts = jnp.concatenate(counts, axis=0).astype(BF16)
        lane_head = lax.rem(lax.broadcasted_iota(jnp.int32, (heads, 128), 1), heads)
        pick = (lane_head == lax.broadcasted_iota(jnp.int32, (heads, 128), 0)).astype(F32).astype(BF16)
        picked = dot_nt(pick, counts).astype(BF16)
        usable = dot_nn(picked, ex[...])

        for h in range(heads):
            us[h] = usable[h : h + 1]
        lanes = lax.broadcasted_iota(jnp.int32, (block_rows, 128), 1)
        stats = jnp.zeros((block_rows, 128), F32)
        own = lax.div(a, per_head)
        for step in sorted(range(heads), key=lambda i: (i == 0, -min(i, heads - i))):
            h = lax.rem(own + step, heads)
            s = jnp.where(us[h] > 0.5, s_ref[h], FLOOR)
            top = jnp.max(s, axis=1, keepdims=True)
            offset = jnp.where(top > 0.5 * FLOOR, top, 0.0)
            p = jnp.exp(s - offset).astype(BF16)
            total = jnp.sum(p.astype(F32), axis=1, keepdims=True)
            safe = jnp.maximum(total, 0.5)
            o = dot_nn(p, vs[h]) / safe
            lse = jnp.where(total > 0.0, offset + jnp.log(safe), FLOOR)
            for i in range(per_head):
                part = slice(i * block_rows, (i + 1) * block_rows)
                o1s[h * per_head + i] = o[part].astype(BF16)
                stats = jnp.where(lanes == h * per_head + i, lse[part], stats)
            for i in range(per_head):
                if step == 0 and i == 0:
                    continue
                t = h * per_head + (lax.rem(a + i, per_head) if step == 0 else i)
                k = step * per_head + i
                r = copy(o1s.at[t], o1r.at[a], o1_send.at[k], o1_recv.at[a], a_dev(lax.rem(t - a + na, na))[1])
                r.start()
                sent.append(r)
        stats = flip(stats)
        for i in range(na):
            l1s[i] = stats[i : i + 1]
        l1r[a] = l1s[a]
        o1r[a] = o1s[a]
        sent += send(a_dev, order_a, lambda t: l1s.at[t], l1r, a, l1_send, l1_recv)
        wait_all(a_dev, order_a, lambda t: l1s.at[t], l1r, na, l1_send, l1_recv)
        w, lse = merge_weights(rows_of(l1r, na))
        w = flip(w)[0:block_rows]
        l2s[...] = lse
        l2r[b] = lse
        sent += send_pairs(l2s, l2r, l2_send, l2_recv)
        wait_all(a_dev, order_a, lambda t: o1s.at[t], o1r, na, o1_send, o1_recv)
        o = w[:, 0:1] * o1r[0].astype(F32)
        for i in range(1, na):
            o = o + w[:, i : i + 1] * o1r[i].astype(F32)
        o = o.astype(BF16)
        o2s[...] = o
        o2r[b] = o
        sent += send_pairs(o2s, o2r, o2_send, o2_recv)
        wait_all(b_dev, order_b, lambda t: l2s, l2r, nb, l2_send, l2_recv)
        w, _ = merge_weights(jnp.concatenate([lf, rows_of(l2r, nb)], axis=0))
        w = flip(w)[0:block_rows]
        o = w[:, 0:1] * of
        wait_all(b_dev, order_b, lambda t: o2s, o2r, nb, o2_send, o2_recv)
        for i in range(nb):
            o = o + w[:, i + 1 : i + 2] * o2r[i].astype(F32)
        o = o.astype(BF16)
        block = jnp.concatenate(
            [o[i * drafts : (i + 1) * drafts] for i in range(width // 128)], axis=1
        )
        fs[...] = block
        fr[a] = block
        sent += send(a_dev, order_a, lambda t: fs, fr, a, f_send, f_recv)
        wait_all(a_dev, order_a, lambda t: fs, fr, na, f_send, f_recv)
        for i in range(na):
            out_ref[:, i * width : (i + 1) * width] = fr[i]
        for r in sent:
            r.wait_send()

    dma = pltpu.SemaphoreType.DMA
    span = heads * 128
    rows = heads * groups * drafts // heads
    scratch = [
        pltpu.VMEM((drafts, heads * groups * 128), BF16),
        pltpu.VMEM((128 // nb // heads, heads), jnp.int32),
        pltpu.VMEM((drafts, span), BF16),
        pltpu.VMEM((drafts, span), BF16),
        dma((4,)),
        pltpu.VMEM((heads, tokens, 128), BF16),
        pltpu.VMEM((heads, tokens, 128), BF16),
        pltpu.VMEM((heads, rows, tokens), F32),
        pltpu.VMEM((1, 128), jnp.int32),
        pltpu.VMEM((nb, 1, 128), jnp.int32),
        pltpu.VMEM((1, 128), jnp.int32),
        pltpu.VMEM((na, 1, 128), jnp.int32),
        pltpu.VMEM((na, block_rows, 128), BF16),
        pltpu.VMEM((na, 1, 128), F32),
        pltpu.VMEM((na, block_rows, 128), BF16),
        pltpu.VMEM((na, 1, 128), F32),
        pltpu.VMEM((block_rows, 128), BF16),
        pltpu.VMEM((1, 128), F32),
        pltpu.VMEM((nb, block_rows, 128), BF16),
        pltpu.VMEM((nb, 1, 128), F32),
        pltpu.VMEM((drafts, width), BF16),
        pltpu.VMEM((na, drafts, width), BF16),
        pltpu.VMEM((128, tokens), BF16),
        pltpu.VMEM((heads, 1, tokens), F32),
        dma((heads,)), dma((heads,)),
        dma((nb,)), dma((nb,)), dma((na,)), dma((na,)),
        dma((na,)), dma((na,)), dma((na,)), dma((na,)),
        dma((nb,)), dma((nb,)), dma((nb,)), dma((nb,)), dma((na,)), dma((na,)),
    ]
    vmem = pl.BlockSpec(memory_space=pltpu.VMEM)
    hbm = pl.BlockSpec(memory_space=pltpu.HBM)
    return pl.pallas_call(
        kernel,
        out_shape=jax.ShapeDtypeStruct((drafts, heads * groups * 128), BF16),
        in_specs=[hbm] * 6,
        out_specs=vmem,
        scratch_shapes=scratch,
        compiler_params=pltpu.CompilerParams(
            collective_id=0, has_side_effects=True, vmem_limit_bytes=52000 * 1024
        ),
    )


def solution(mesh):
    nz, nx, nc = 16, 4, 2
    torus = Mesh(
        mesh.devices.reshape(mesh.shape["grp"], nz, nx, nc), ("grp", "page_0", "page_1", "page_2")
    )

    def on_device(queries, key_cache, value_cache, new_keys, new_values, chosen):
        pages, page_tokens, span = key_cache.shape
        heads = chosen.shape[0]
        drafts = queries.shape[0]
        groups = queries.shape[1] // span
        call = make_kernel(
            nz, nx, nc, heads, pages * page_tokens, page_tokens, drafts, groups,
            (span // heads) ** (-0.5),
        )
        return call(
            queries, chosen.T, new_keys, new_values,
            key_cache.reshape(-1, span), value_cache.reshape(-1, span),
        )

    in_specs = (
        P("grp", None),
        P(GRP_PAGE, None, None),
        P(GRP_PAGE, None, None),
        P("grp", None),
        P("grp", None),
        P("grp", PAGE),
    )
    return jax.shard_map(
        on_device, mesh=torus, in_specs=in_specs, out_specs=P("grp", None), check_vma=False
    )
```

```python
import jax
import jax.numpy as jnp
from jax import lax
from jax.experimental import pallas as pl
from jax.experimental.pallas import tpu as pltpu
from jax.sharding import Mesh
from jax.sharding import PartitionSpec as P

GRP_PAGE = ("grp", "page_0", "page_1", "page_2")
PAGE = GRP_PAGE[1:]
FLOOR = -1e30
F32 = jnp.float32
BF16 = jnp.bfloat16
MESH = pl.DeviceIdType.MESH


def dot_nt(a, b):
    return lax.dot_general(a, b, (((1,), (1,)), ((), ())), preferred_element_type=F32)


def dot_nn(a, b):
    return lax.dot_general(a, b, (((1,), (0,)), ((), ())), preferred_element_type=F32)


def rows_of(ref, count):
    return jnp.concatenate([ref[i] for i in range(count)], axis=0)


def flip(x):
    n = x.shape[0]
    if n < 128:
        x = jnp.concatenate([x, jnp.zeros((128 - n, 128), x.dtype)], axis=0)
    return jnp.transpose(x)


def merge_weights(lse):
    top = jnp.max(lse, axis=0, keepdims=True)
    w = jnp.exp(lse - top)
    total = jnp.sum(w, axis=0, keepdims=True)
    return w / total, top + jnp.log(total)


def far_first(n, ring):
    def key(d):
        return -min(d // ring, (n - d) // ring)

    return sorted(range(1, n), key=key)


def make_kernel(nz, nx, nc, heads, tokens, page_tokens, drafts, groups, scaling):
    na = nx * nc * 2
    nb = nz // 2
    pages = tokens // page_tokens
    block_rows = heads * groups * drafts // na
    per_head = na // heads
    width = block_rows // drafts * 128

    def kernel(
        q_hbm, ids_hbm, nk_hbm, nv_hbm, k_hbm, v_hbm, out_ref,
        q_ref, ids_ref, nk_ref, nv_ref, small_sem, ks, vs, s_ref, idbs, idbr, idas, idar,
        o1s, l1s, o1r, l1r, o2s, l2s, o2r, l2r, fs, fr, ex,
        k_sem, v_sem, b_send, b_recv, a_send, a_recv,
        o1_send, o1_recv, l1_send, l1_recv,
        o2_send, o2_recv, l2_send, l2_recv, f_send, f_recv,
    ):
        z = lax.axis_index("page_0")
        x = lax.axis_index("page_1")
        c = lax.axis_index("page_2")
        zlow = lax.rem(z, 2)
        b = lax.div(z, 2)
        a = (x * nc + c) * 2 + zlow

        def a_dev(d):
            t = lax.rem(a + d, na)
            u = lax.div(t, 2)
            return t, {
                "page_0": b * 2 + lax.rem(t, 2),
                "page_1": lax.div(u, nc),
                "page_2": lax.rem(u, nc),
            }

        def b_dev(d):
            t = lax.rem(b + d, nb)
            return t, {"page_0": t * 2 + zlow, "page_1": x, "page_2": c}

        order_a = far_first(na, nc * 2)
        order_b = far_first(nb, 1)

        def copy(src, dst, ss, rs, dev):
            return pltpu.make_async_remote_copy(
                src_ref=src, dst_ref=dst, send_sem=ss, recv_sem=rs,
                device_id=dev, device_id_type=MESH,
            )

        def send(group, order, src, dst, me, ss, rs):
            for d in order:
                t, dev = group(d)
                copy(src(t), dst.at[me], ss, rs, dev).start()

        def wait_bytes(buf, count, sem):
            part = buf.at[pl.ds(0, count)]
            pltpu.make_async_copy(part, part, sem).wait()

        small = [
            pltpu.make_async_copy(src, dst, small_sem.at[i])
            for i, (src, dst) in enumerate(
                [(ids_hbm, ids_ref), (q_hbm, q_ref), (nk_hbm, nk_ref), (nv_hbm, nv_ref)]
            )
        ]
        small[0].start()
        def send_pairs(src, dst, ss, rs):
            for t in range(nb):
                d = lax.rem(t - b + nb, nb)

                @pl.when(d != 0)
                def _():
                    copy(src, dst.at[b], ss, rs, b_dev(d)[1]).start()

        barrier = pltpu.get_barrier_semaphore()
        for d in order_b:
            pl.semaphore_signal(barrier, inc=1, device_id=b_dev(d)[1], device_id_type=MESH)
        for d in order_a:
            pl.semaphore_signal(barrier, inc=1, device_id=a_dev(d)[1], device_id_type=MESH)

        def load(src, dst, sem, h):
            return pltpu.make_async_copy(src.at[:, pl.ds(h * 128, 128)], dst.at[h], sem)

        for r in small[1:]:
            r.start()
        for h in range(heads):
            load(k_hbm, ks, k_sem, h).start()
        for h in range(heads):
            load(v_hbm, vs, v_sem, h).start()

        lane = lax.broadcasted_iota(jnp.int32, (1, 128), 1)
        slot = 128 // nb
        small[0].wait()
        ids = ids_ref[...]
        ids = jnp.concatenate([ids[j : j + 1] for j in range(ids.shape[0])] * nb, axis=1)
        idbs[...] = jnp.where(lax.div(lane, slot) == b, ids, 0)
        idbr[b] = idbs[...]

        def scores(h):
            base = h * groups * 128
            q = jnp.concatenate(
                [q_ref[:, base + g * 128 : base + (g + 1) * 128] for g in range(groups)], axis=0
            )
            s_ref[h] = dot_nt(q, ks[h]) * scaling

        pl.semaphore_wait(barrier, na - 1 + nb - 1)
        send(b_dev, order_b, lambda t: idbs, idbr, b, b_send, b_recv)
        for r in small[1:]:
            r.wait()
        wait_bytes(ks, heads, k_sem)
        for h in range(heads):
            scores(h)

        cols = pl.multiple_of(a * width, width)
        head_cols = pl.multiple_of(lax.div(a, per_head) * 128, 128)
        q_own = q_ref[:, pl.ds(cols, width)]
        q_own = jnp.concatenate(
            [q_own[:, i * 128 : (i + 1) * 128] for i in range(width // 128)], axis=0
        )
        pad = jnp.zeros((128 - drafts, 128), BF16)
        kf = jnp.concatenate([nk_ref[:, pl.ds(head_cols, 128)], pad], axis=0)
        vf = jnp.concatenate([nv_ref[:, pl.ds(head_cols, 128)], pad], axis=0)
        sf = dot_nt(q_own, kf) * scaling
        pos = lax.rem(lax.broadcasted_iota(jnp.int32, sf.shape, 0), drafts)
        ok = lax.broadcasted_iota(jnp.int32, sf.shape, 1) <= pos
        sf = jnp.where(ok, sf, FLOOR)
        mf = jnp.max(sf, axis=1, keepdims=True)
        pf = jnp.where(ok, jnp.exp(sf - mf), 0.0).astype(BF16)
        tf = jnp.sum(pf.astype(F32), axis=1, keepdims=True)
        of = dot_nn(pf, vf) / tf
        lf = flip(jnp.broadcast_to(mf + jnp.log(tf), (block_rows, 128)))[0:1]

        key_page = lax.div(lax.broadcasted_iota(jnp.int32, (128, tokens), 1), page_tokens)
        row_page = lax.broadcasted_iota(jnp.int32, (128, tokens), 0)
        ex[...] = (key_page == row_page).astype(F32).astype(BF16)

        wait_bytes(idbr, nb - 1, b_recv)
        joined = idbr[0]
        for i in range(1, nb):
            joined = joined + idbr[i]
        idas[...] = joined
        idar[a] = joined
        send(a_dev, order_a, lambda t: idas, idar, a, a_send, a_recv)
        wait_bytes(vs, heads, v_sem)
        wait_bytes(idar, na - 1, a_recv)

        local = rows_of(idar, na) - ((z * nx + x) * nc + c) * pages
        counts = [
            jnp.sum((local == p).astype(F32), axis=0, keepdims=True) for p in range(pages)
        ]
        counts.append(jnp.zeros((128 - pages, 128), F32))
        counts = jnp.concatenate(counts, axis=0).astype(BF16)
        lane_head = lax.rem(lax.broadcasted_iota(jnp.int32, (heads, 128), 1), heads)
        pick = (lane_head == lax.broadcasted_iota(jnp.int32, (heads, 128), 0)).astype(F32).astype(BF16)
        picked = dot_nt(pick, counts).astype(BF16)
        usable = dot_nn(picked, ex[...])

        lanes = lax.broadcasted_iota(jnp.int32, (block_rows, 128), 1)
        stats = jnp.zeros((block_rows, 128), F32)
        for h in range(heads):
            s = jnp.where(usable[h : h + 1] > 0.5, s_ref[h], FLOOR)
            top = jnp.max(s, axis=1, keepdims=True)
            offset = jnp.where(top > 0.5 * FLOOR, top, 0.0)
            p = jnp.exp(s - offset).astype(BF16)
            total = jnp.sum(p.astype(F32), axis=1, keepdims=True)
            safe = jnp.maximum(total, 0.5)
            o = dot_nn(p, vs[h]) / safe
            lse = jnp.where(total > 0.0, offset + jnp.log(safe), FLOOR)
            for i in range(per_head):
                part = slice(i * block_rows, (i + 1) * block_rows)
                o1s[h * per_head + i] = o[part].astype(BF16)
                stats = jnp.where(lanes == h * per_head + i, lse[part], stats)
        send(a_dev, order_a, lambda t: o1s.at[t], o1r, a, o1_send, o1_recv)
        o1r[a] = o1s[a]
        stats = flip(stats)
        for i in range(na):
            l1s[i] = stats[i : i + 1]
        l1r[a] = l1s[a]
        send(a_dev, order_a, lambda t: l1s.at[t], l1r, a, l1_send, l1_recv)
        wait_bytes(l1r, na - 1, l1_recv)
        w, lse = merge_weights(rows_of(l1r, na))
        w = flip(w)[0:block_rows]
        l2s[...] = lse
        l2r[b] = lse
        send_pairs(l2s, l2r, l2_send, l2_recv)
        wait_bytes(o1r, na - 1, o1_recv)
        o = w[:, 0:1] * o1r[0].astype(F32)
        for i in range(1, na):
            o = o + w[:, i : i + 1] * o1r[i].astype(F32)
        o = o.astype(BF16)
        o2s[...] = o
        o2r[b] = o
        send_pairs(o2s, o2r, o2_send, o2_recv)
        wait_bytes(l2r, nb - 1, l2_recv)
        w, _ = merge_weights(jnp.concatenate([lf, rows_of(l2r, nb)], axis=0))
        w = flip(w)[0:block_rows]
        o = w[:, 0:1] * of
        wait_bytes(o2r, nb - 1, o2_recv)
        for i in range(nb):
            o = o + w[:, i + 1 : i + 2] * o2r[i].astype(F32)
        o = o.astype(BF16)
        block = jnp.concatenate(
            [o[i * drafts : (i + 1) * drafts] for i in range(width // 128)], axis=1
        )
        fs[...] = block
        fr[a] = block
        send(a_dev, order_a, lambda t: fs, fr, a, f_send, f_recv)
        wait_bytes(fr, na - 1, f_recv)
        for i in range(na):
            out_ref[:, i * width : (i + 1) * width] = fr[i]
        wait_bytes(idbr, nb - 1, b_send)
        wait_bytes(idar, na - 1, a_send)
        wait_bytes(o1r, na - 1, o1_send)
        wait_bytes(l1r, na - 1, l1_send)
        wait_bytes(o2r, nb - 1, o2_send)
        wait_bytes(l2r, nb - 1, l2_send)
        wait_bytes(fr, na - 1, f_send)

    dma = pltpu.SemaphoreType.DMA
    span = heads * 128
    rows = heads * groups * drafts // heads
    scratch = [
        pltpu.VMEM((drafts, heads * groups * 128), BF16),
        pltpu.VMEM((128 // nb // heads, heads), jnp.int32),
        pltpu.VMEM((drafts, span), BF16),
        pltpu.VMEM((drafts, span), BF16),
        dma((4,)),
        pltpu.VMEM((heads, tokens, 128), BF16),
        pltpu.VMEM((heads, tokens, 128), BF16),
        pltpu.VMEM((heads, rows, tokens), F32),
        pltpu.VMEM((1, 128), jnp.int32),
        pltpu.VMEM((nb, 1, 128), jnp.int32),
        pltpu.VMEM((1, 128), jnp.int32),
        pltpu.VMEM((na, 1, 128), jnp.int32),
        pltpu.VMEM((na, block_rows, 128), BF16),
        pltpu.VMEM((na, 1, 128), F32),
        pltpu.VMEM((na, block_rows, 128), BF16),
        pltpu.VMEM((na, 1, 128), F32),
        pltpu.VMEM((block_rows, 128), BF16),
        pltpu.VMEM((1, 128), F32),
        pltpu.VMEM((nb, block_rows, 128), BF16),
        pltpu.VMEM((nb, 1, 128), F32),
        pltpu.VMEM((drafts, width), BF16),
        pltpu.VMEM((na, drafts, width), BF16),
        pltpu.VMEM((128, tokens), BF16),
        *[dma] * 16,
    ]
    vmem = pl.BlockSpec(memory_space=pltpu.VMEM)
    hbm = pl.BlockSpec(memory_space=pltpu.HBM)
    return pl.pallas_call(
        kernel,
        out_shape=jax.ShapeDtypeStruct((drafts, heads * groups * 128), BF16),
        in_specs=[hbm] * 6,
        out_specs=vmem,
        scratch_shapes=scratch,
        compiler_params=pltpu.CompilerParams(
            collective_id=0, has_side_effects=True, vmem_limit_bytes=32 * 1024 * 1024
        ),
    )


def solution(mesh):
    nz, nx, nc = 16, 4, 2
    torus = Mesh(
        mesh.devices.reshape(mesh.shape["grp"], nz, nx, nc), ("grp", "page_0", "page_1", "page_2")
    )

    def on_device(queries, key_cache, value_cache, new_keys, new_values, chosen):
        pages, page_tokens, span = key_cache.shape
        heads = chosen.shape[0]
        drafts = queries.shape[0]
        groups = queries.shape[1] // span
        call = make_kernel(
            nz, nx, nc, heads, pages * page_tokens, page_tokens, drafts, groups,
            (span // heads) ** (-0.5),
        )
        return call(
            *[
                pltpu.with_memory_space_constraint(x, pltpu.HBM)
                for x in (
                    queries, chosen.T, new_keys, new_values,
                    key_cache.reshape(-1, span), value_cache.reshape(-1, span),
                )
            ]
        )

    in_specs = (
        P("grp", None),
        P(GRP_PAGE, None, None),
        P(GRP_PAGE, None, None),
        P("grp", None),
        P("grp", None),
        P("grp", PAGE),
    )
    return jax.shard_map(
        on_device, mesh=torus, in_specs=in_specs, out_specs=P("grp", None), check_vma=False
    )
```

```python
import jax
import jax.numpy as jnp
from jax import lax
from jax.experimental import pallas as pl
from jax.experimental.pallas import tpu as pltpu
from jax.sharding import Mesh
from jax.sharding import PartitionSpec as P

GRP_PAGE = ("grp", "page_0", "page_1", "page_2")
PAGE = GRP_PAGE[1:]
FLOOR = -1e30
F32 = jnp.float32
BF16 = jnp.bfloat16
MESH = pl.DeviceIdType.MESH


def dot_nt(a, b):
    return lax.dot_general(a, b, (((1,), (1,)), ((), ())), preferred_element_type=F32)


def dot_nn(a, b):
    return lax.dot_general(a, b, (((1,), (0,)), ((), ())), preferred_element_type=F32)


def rows_of(ref, count):
    return jnp.concatenate([ref[i] for i in range(count)], axis=0)


def flip(x):
    n = x.shape[0]
    if n < 128:
        x = jnp.concatenate([x, jnp.zeros((128 - n, 128), x.dtype)], axis=0)
    return jnp.transpose(x)


def merge_weights(lse):
    top = jnp.max(lse, axis=0, keepdims=True)
    w = jnp.exp(lse - top)
    total = jnp.sum(w, axis=0, keepdims=True)
    return w / total, top + jnp.log(total)


def far_first(n, ring):
    def key(d):
        return -min(d // ring, (n - d) // ring)

    return sorted(range(1, n), key=key)


def make_kernel(nz, nx, nc, heads, tokens, page_tokens, drafts, groups, scaling):
    na = nx * nc * 2
    nb = nz // 2
    pages = tokens // page_tokens
    block_rows = heads * groups * drafts // na
    per_head = na // heads
    width = block_rows // drafts * 128

    def kernel(
        q_hbm, ids_hbm, nk_hbm, nv_hbm, k_hbm, v_hbm, out_ref,
        q_ref, ids_ref, nk_ref, nv_ref, small_sem, ks, vs, s_ref, ups, upr, idbs, idbr, idas, idar,
        o1s, l1s, o1r, l1r, o2s, l2s, o2r, l2r, fs, fr, ex,
        k_sem, v_sem, up_send, up_recv, b_send, b_recv, a_send, a_recv,
        o1_send, o1_recv, l1_send, l1_recv,
        o2_send, o2_recv, l2_send, l2_recv, f_send, f_recv,
    ):
        z = lax.axis_index("page_0")
        x = lax.axis_index("page_1")
        c = lax.axis_index("page_2")
        zlow = lax.rem(z, 2)
        b = lax.div(z, 2)
        a = (x * nc + c) * 2 + zlow

        def a_dev(d):
            t = lax.rem(a + d, na)
            u = lax.div(t, 2)
            return t, {
                "page_0": b * 2 + lax.rem(t, 2),
                "page_1": lax.div(u, nc),
                "page_2": lax.rem(u, nc),
            }

        def b_dev(d):
            t = lax.rem(b + d, nb)
            return t, {"page_0": t * 2 + zlow, "page_1": x, "page_2": c}

        def pair_dev(t):
            return {"page_0": t * 2 + zlow, "page_1": x, "page_2": c}

        order_a = far_first(na, nc * 2)
        order_b = far_first(nb, 1)

        def copy(src, dst, ss, rs, dev):
            return pltpu.make_async_remote_copy(
                src_ref=src, dst_ref=dst, send_sem=ss, recv_sem=rs,
                device_id=dev, device_id_type=MESH,
            )

        def send(group, order, src, dst, me, ss, rs):
            for d in order:
                t, dev = group(d)
                copy(src(t), dst.at[me], ss, rs, dev).start()

        def wait_bytes(buf, count, sem):
            part = buf.at[pl.ds(0, count)]
            pltpu.make_async_copy(part, part, sem).wait()

        small = [
            pltpu.make_async_copy(src, dst, small_sem.at[i])
            for i, (src, dst) in enumerate(
                [(ids_hbm, ids_ref), (q_hbm, q_ref), (nk_hbm, nk_ref), (nv_hbm, nv_ref)]
            )
        ]
        small[0].start()

        def send_pairs(src, dst, ss, rs):
            for t in range(nb):
                d = lax.rem(t - b + nb, nb)

                @pl.when(d != 0)
                def _():
                    copy(src, dst.at[b], ss, rs, b_dev(d)[1]).start()

        barrier = pltpu.get_barrier_semaphore()
        for d in order_a:
            pl.semaphore_signal(barrier, inc=1, device_id=a_dev(d)[1], device_id_type=MESH)
        for t in range(nb):

            @pl.when((t == b - 1) | (t > b))
            def _():
                pl.semaphore_signal(barrier, inc=1, device_id=pair_dev(t), device_id_type=MESH)

        def load(src, dst, sem, h):
            return pltpu.make_async_copy(src.at[:, pl.ds(h * 128, 128)], dst.at[h], sem)

        for r in small[1:]:
            r.start()
        for h in range(heads):
            load(k_hbm, ks, k_sem, h).start()
        for h in range(heads):
            load(v_hbm, vs, v_sem, h).start()

        lane = lax.broadcasted_iota(jnp.int32, (1, 128), 1)
        slot = 128 // nb
        small[0].wait()
        ids = ids_ref[...]
        ids = jnp.concatenate([ids[j : j + 1] for j in range(ids.shape[0])] * nb, axis=1)
        idbs[...] = jnp.where(lax.div(lane, slot) == b, ids, 0)
        for t in range(nb):

            @pl.when(t <= b)
            def _():
                idbr[t] = jnp.zeros((1, 128), jnp.int32)

        @pl.when(b == 0)
        def _():
            upr[...] = jnp.zeros((1, 128), jnp.int32)


        def scores(h):
            base = h * groups * 128
            q = jnp.concatenate(
                [q_ref[:, base + g * 128 : base + (g + 1) * 128] for g in range(groups)], axis=0
            )
            s_ref[h] = dot_nt(q, ks[h]) * scaling

        def all_scores():
            small[1].wait()
            wait_bytes(ks, heads, k_sem)
            for h in range(heads):
                scores(h)

        def up():
            return copy(ups, upr, up_send, up_recv, pair_dev(lax.rem(b + 1, nb)))

        def down(t):
            return copy(idbs, idbr.at[b], b_send.at[t], b_recv.at[b], pair_dev(t))

        early = b < nb - 3

        @pl.when(early)
        def _():
            all_scores()

        pl.semaphore_wait(barrier, na - 1 + b + (b < nb - 1).astype(jnp.int32))
        for t in range(nb):

            @pl.when(t < b)
            def _():
                down(t).start()

        @pl.when(jnp.logical_not(early))
        def _():
            all_scores()

        @pl.when(b > 0)
        def _():
            up().wait_recv()

        ups[...] = upr[...] + idbs[...]

        @pl.when(b < nb - 1)
        def _():
            up().start()

        for r in small[2:]:
            r.wait()
        cols = pl.multiple_of(a * width, width)
        head_cols = pl.multiple_of(lax.div(a, per_head) * 128, 128)
        q_own = q_ref[:, pl.ds(cols, width)]
        q_own = jnp.concatenate(
            [q_own[:, i * 128 : (i + 1) * 128] for i in range(width // 128)], axis=0
        )
        pad = jnp.zeros((128 - drafts, 128), BF16)
        kf = jnp.concatenate([nk_ref[:, pl.ds(head_cols, 128)], pad], axis=0)
        vf = jnp.concatenate([nv_ref[:, pl.ds(head_cols, 128)], pad], axis=0)
        sf = dot_nt(q_own, kf) * scaling
        pos = lax.rem(lax.broadcasted_iota(jnp.int32, sf.shape, 0), drafts)
        ok = lax.broadcasted_iota(jnp.int32, sf.shape, 1) <= pos
        sf = jnp.where(ok, sf, FLOOR)
        mf = jnp.max(sf, axis=1, keepdims=True)
        pf = jnp.where(ok, jnp.exp(sf - mf), 0.0).astype(BF16)
        tf = jnp.sum(pf.astype(F32), axis=1, keepdims=True)
        of = dot_nn(pf, vf) / tf
        lf = flip(jnp.broadcast_to(mf + jnp.log(tf), (block_rows, 128)))[0:1]

        key_page = lax.div(lax.broadcasted_iota(jnp.int32, (128, tokens), 1), page_tokens)
        row_page = lax.broadcasted_iota(jnp.int32, (128, tokens), 0)
        ex[...] = (key_page == row_page).astype(F32).astype(BF16)

        for t in range(nb):

            @pl.when(t > b)
            def _():
                copy(idbs, idbr.at[t], b_send.at[t], b_recv.at[t], pair_dev(t)).wait_recv()

        joined = ups[...]
        for i in range(nb):
            joined = joined + idbr[i]
        idas[...] = joined
        idar[a] = joined
        send(a_dev, order_a, lambda t: idas, idar, a, a_send, a_recv)
        wait_bytes(vs, heads, v_sem)
        wait_bytes(idar, na - 1, a_recv)

        local = rows_of(idar, na) - ((z * nx + x) * nc + c) * pages
        counts = [
            jnp.sum((local == p).astype(F32), axis=0, keepdims=True) for p in range(pages)
        ]
        counts.append(jnp.zeros((128 - pages, 128), F32))
        counts = jnp.concatenate(counts, axis=0).astype(BF16)
        lane_head = lax.rem(lax.broadcasted_iota(jnp.int32, (heads, 128), 1), heads)
        pick = (lane_head == lax.broadcasted_iota(jnp.int32, (heads, 128), 0)).astype(F32).astype(BF16)
        picked = dot_nt(pick, counts).astype(BF16)
        usable = dot_nn(picked, ex[...])

        lanes = lax.broadcasted_iota(jnp.int32, (block_rows, 128), 1)
        stats = jnp.zeros((block_rows, 128), F32)
        for h in range(heads):
            s = jnp.where(usable[h : h + 1] > 0.5, s_ref[h], FLOOR)
            top = jnp.max(s, axis=1, keepdims=True)
            offset = jnp.where(top > 0.5 * FLOOR, top, 0.0)
            p = jnp.exp(s - offset).astype(BF16)
            total = jnp.sum(p.astype(F32), axis=1, keepdims=True)
            safe = jnp.maximum(total, 0.5)
            o = dot_nn(p, vs[h]) / safe
            lse = jnp.where(total > 0.0, offset + jnp.log(safe), FLOOR)
            for i in range(per_head):
                part = slice(i * block_rows, (i + 1) * block_rows)
                o1s[h * per_head + i] = o[part].astype(BF16)
                stats = jnp.where(lanes == h * per_head + i, lse[part], stats)
        stats = flip(stats)
        for i in range(na):
            l1s[i] = stats[i : i + 1]
        l1r[a] = l1s[a]
        send(a_dev, order_a, lambda t: l1s.at[t], l1r, a, l1_send, l1_recv)
        send(a_dev, order_a, lambda t: o1s.at[t], o1r, a, o1_send, o1_recv)
        o1r[a] = o1s[a]
        wait_bytes(l1r, na - 1, l1_recv)
        w, lse = merge_weights(rows_of(l1r, na))
        w = flip(w)[0:block_rows]
        l2s[...] = lse
        l2r[b] = lse
        send_pairs(l2s, l2r, l2_send, l2_recv)
        wait_bytes(o1r, na - 1, o1_recv)
        o = w[:, 0:1] * o1r[0].astype(F32)
        for i in range(1, na):
            o = o + w[:, i : i + 1] * o1r[i].astype(F32)
        o = o.astype(BF16)
        o2s[...] = o
        o2r[b] = o
        send_pairs(o2s, o2r, o2_send, o2_recv)
        wait_bytes(l2r, nb - 1, l2_recv)
        w, _ = merge_weights(jnp.concatenate([lf, rows_of(l2r, nb)], axis=0))
        w = flip(w)[0:block_rows]
        o = w[:, 0:1] * of
        wait_bytes(o2r, nb - 1, o2_recv)
        for i in range(nb):
            o = o + w[:, i + 1 : i + 2] * o2r[i].astype(F32)
        o = o.astype(BF16)
        block = jnp.concatenate(
            [o[i * drafts : (i + 1) * drafts] for i in range(width // 128)], axis=1
        )
        fs[...] = block
        fr[a] = block
        send(a_dev, order_a, lambda t: fs, fr, a, f_send, f_recv)
        wait_bytes(fr, na - 1, f_recv)
        for i in range(na):
            out_ref[:, i * width : (i + 1) * width] = fr[i]
        for t in range(nb):

            @pl.when(t < b)
            def _():
                down(t).wait_send()

        @pl.when(b < nb - 1)
        def _():
            up().wait_send()

        wait_bytes(idar, na - 1, a_send)
        wait_bytes(o1r, na - 1, o1_send)
        wait_bytes(l1r, na - 1, l1_send)
        wait_bytes(o2r, nb - 1, o2_send)
        wait_bytes(l2r, nb - 1, l2_send)
        wait_bytes(fr, na - 1, f_send)

    dma = pltpu.SemaphoreType.DMA
    span = heads * 128
    rows = heads * groups * drafts // heads
    scratch = [
        pltpu.VMEM((drafts, heads * groups * 128), BF16),
        pltpu.VMEM((128 // nb // heads, heads), jnp.int32),
        pltpu.VMEM((drafts, span), BF16),
        pltpu.VMEM((drafts, span), BF16),
        dma((4,)),
        pltpu.VMEM((heads, tokens, 128), BF16),
        pltpu.VMEM((heads, tokens, 128), BF16),
        pltpu.VMEM((heads, rows, tokens), F32),
        pltpu.VMEM((1, 128), jnp.int32),
        pltpu.VMEM((1, 128), jnp.int32),
        pltpu.VMEM((1, 128), jnp.int32),
        pltpu.VMEM((nb, 1, 128), jnp.int32),
        pltpu.VMEM((1, 128), jnp.int32),
        pltpu.VMEM((na, 1, 128), jnp.int32),
        pltpu.VMEM((na, block_rows, 128), BF16),
        pltpu.VMEM((na, 1, 128), F32),
        pltpu.VMEM((na, block_rows, 128), BF16),
        pltpu.VMEM((na, 1, 128), F32),
        pltpu.VMEM((block_rows, 128), BF16),
        pltpu.VMEM((1, 128), F32),
        pltpu.VMEM((nb, block_rows, 128), BF16),
        pltpu.VMEM((nb, 1, 128), F32),
        pltpu.VMEM((drafts, width), BF16),
        pltpu.VMEM((na, drafts, width), BF16),
        pltpu.VMEM((128, tokens), BF16),
        *[dma] * 4, dma((nb,)), dma((nb,)), *[dma] * 12,
    ]
    vmem = pl.BlockSpec(memory_space=pltpu.VMEM)
    hbm = pl.BlockSpec(memory_space=pltpu.HBM)
    return pl.pallas_call(
        kernel,
        out_shape=jax.ShapeDtypeStruct((drafts, heads * groups * 128), BF16),
        in_specs=[hbm] * 6,
        out_specs=vmem,
        scratch_shapes=scratch,
        compiler_params=pltpu.CompilerParams(
            collective_id=0, has_side_effects=True, vmem_limit_bytes=32 * 1024 * 1024
        ),
    )


def solution(mesh):
    nz, nx, nc = 16, 4, 2
    torus = Mesh(
        mesh.devices.reshape(mesh.shape["grp"], nz, nx, nc), ("grp", "page_0", "page_1", "page_2")
    )

    def on_device(queries, key_cache, value_cache, new_keys, new_values, chosen):
        pages, page_tokens, span = key_cache.shape
        heads = chosen.shape[0]
        drafts = queries.shape[0]
        groups = queries.shape[1] // span
        call = make_kernel(
            nz, nx, nc, heads, pages * page_tokens, page_tokens, drafts, groups,
            (span // heads) ** (-0.5),
        )
        return call(
            *[
                pltpu.with_memory_space_constraint(x, pltpu.HBM)
                for x in (
                    queries, chosen.T, new_keys, new_values,
                    key_cache.reshape(-1, span), value_cache.reshape(-1, span),
                )
            ]
        )

    in_specs = (
        P("grp", None),
        P(GRP_PAGE, None, None),
        P(GRP_PAGE, None, None),
        P("grp", None),
        P("grp", None),
        P("grp", PAGE),
    )
    return jax.shard_map(
        on_device, mesh=torus, in_specs=in_specs, out_specs=P("grp", None), check_vma=False
    )
```

```python
import jax
import jax.numpy as jnp
from jax import lax
from jax.experimental import pallas as pl
from jax.experimental.pallas import tpu as pltpu
from jax.sharding import Mesh
from jax.sharding import PartitionSpec as P

GRP_PAGE = ("grp", "page_0", "page_1", "page_2")
PAGE = GRP_PAGE[1:]
FLOOR = -1e30
F32 = jnp.float32
BF16 = jnp.bfloat16
MESH = pl.DeviceIdType.MESH


def dot_nt(a, b):
    return lax.dot_general(a, b, (((1,), (1,)), ((), ())), preferred_element_type=F32)


def dot_nn(a, b):
    return lax.dot_general(a, b, (((1,), (0,)), ((), ())), preferred_element_type=F32)


def rows_of(ref, count):
    return jnp.concatenate([ref[i] for i in range(count)], axis=0)


def flip(x):
    n = x.shape[0]
    if n < 128:
        x = jnp.concatenate([x, jnp.zeros((128 - n, 128), x.dtype)], axis=0)
    return jnp.transpose(x)


def merge_weights(lse):
    top = jnp.max(lse, axis=0, keepdims=True)
    w = jnp.exp(lse - top)
    total = jnp.sum(w, axis=0, keepdims=True)
    return w / total, top + jnp.log(total)


def far_first(n, ring):
    def key(d):
        return -min(d // ring, (n - d) // ring)

    return sorted(range(1, n), key=key)


def make_kernel(nz, nx, nc, heads, tokens, page_tokens, drafts, groups, scaling):
    na = nx * nc * 2
    nb = nz // 2
    pages = tokens // page_tokens
    block_rows = heads * groups * drafts // na
    per_head = na // heads
    width = block_rows // drafts * 128

    def kernel(
        q_hbm, ids_hbm, nk_hbm, nv_hbm, k_hbm, v_hbm, out_ref,
        q_ref, ids_ref, nk_ref, nv_ref, small_sem, ks, vs, s_ref, idbs, idbr, idas, idar,
        o1s, l1s, o1r, l1r, o2s, l2s, o2r, l2r, fs, fr, ex,
        k_sem, v_sem, b_send, b_recv, a_send, a_recv,
        o1_send, o1_recv, l1_send, l1_recv,
        o2_send, o2_recv, l2_send, l2_recv, f_send, f_recv,
    ):
        z = lax.axis_index("page_0")
        x = lax.axis_index("page_1")
        c = lax.axis_index("page_2")
        zlow = lax.rem(z, 2)
        b = lax.div(z, 2)
        a = (x * nc + c) * 2 + zlow

        def a_dev(d):
            t = lax.rem(a + d, na)
            u = lax.div(t, 2)
            return t, {
                "page_0": b * 2 + lax.rem(t, 2),
                "page_1": lax.div(u, nc),
                "page_2": lax.rem(u, nc),
            }

        def b_dev(d):
            t = lax.rem(b + d, nb)
            return t, {"page_0": t * 2 + zlow, "page_1": x, "page_2": c}

        order_a = far_first(na, nc * 2)
        order_b = far_first(nb, 1)

        def copy(src, dst, ss, rs, dev):
            return pltpu.make_async_remote_copy(
                src_ref=src, dst_ref=dst, send_sem=ss, recv_sem=rs,
                device_id=dev, device_id_type=MESH,
            )

        def send(group, order, src, dst, me, ss, rs):
            for d in order:
                t, dev = group(d)
                copy(src(t), dst.at[me], ss, rs, dev).start()

        def wait_bytes(buf, count, sem):
            part = buf.at[pl.ds(0, count)]
            pltpu.make_async_copy(part, part, sem).wait()

        small = [
            pltpu.make_async_copy(src, dst, small_sem.at[i])
            for i, (src, dst) in enumerate(
                [(ids_hbm, ids_ref), (q_hbm, q_ref), (nk_hbm, nk_ref), (nv_hbm, nv_ref)]
            )
        ]
        small[0].start()

        def send_pairs(targets, src, dst, ss, rs):
            for t in targets:
                d = lax.rem(t - b + nb, nb)

                @pl.when(d != 0)
                def _():
                    copy(src, dst.at[b], ss, rs, b_dev(d)[1]).start()

        barrier = pltpu.get_barrier_semaphore()
        for d in order_b:
            pl.semaphore_signal(barrier, inc=1, device_id=b_dev(d)[1], device_id_type=MESH)
        for d in order_a:
            pl.semaphore_signal(barrier, inc=1, device_id=a_dev(d)[1], device_id_type=MESH)

        def load(src, dst, sem, h):
            return pltpu.make_async_copy(src.at[:, pl.ds(h * 128, 128)], dst.at[h], sem)

        for r in small[1:]:
            r.start()
        for h in range(heads):
            load(k_hbm, ks, k_sem, h).start()
        for h in range(heads):
            load(v_hbm, vs, v_sem, h).start()

        lane = lax.broadcasted_iota(jnp.int32, (1, 128), 1)
        slot = 128 // nb
        small[0].wait()
        ids = ids_ref[...]
        ids = jnp.concatenate([ids[j : j + 1] for j in range(ids.shape[0])] * nb, axis=1)
        idbs[...] = jnp.where(lax.div(lane, slot) == b, ids, 0)
        idbr[b] = idbs[...]

        def scores(h):
            base = h * groups * 128
            q = jnp.concatenate(
                [q_ref[:, base + g * 128 : base + (g + 1) * 128] for g in range(groups)], axis=0
            )
            s_ref[h] = dot_nt(q, ks[h]) * scaling

        pl.semaphore_wait(barrier, na - 1 + nb - 1)
        send(b_dev, order_b, lambda t: idbs, idbr, b, b_send, b_recv)
        for r in small[1:]:
            r.wait()
        wait_bytes(ks, heads, k_sem)
        for h in range(heads):
            scores(h)

        cols = pl.multiple_of(a * width, width)
        head_cols = pl.multiple_of(lax.div(a, per_head) * 128, 128)
        q_own = q_ref[:, pl.ds(cols, width)]
        q_own = jnp.concatenate(
            [q_own[:, i * 128 : (i + 1) * 128] for i in range(width // 128)], axis=0
        )
        pad = jnp.zeros((128 - drafts, 128), BF16)
        kf = jnp.concatenate([nk_ref[:, pl.ds(head_cols, 128)], pad], axis=0)
        vf = jnp.concatenate([nv_ref[:, pl.ds(head_cols, 128)], pad], axis=0)
        sf = dot_nt(q_own, kf) * scaling
        pos = lax.rem(lax.broadcasted_iota(jnp.int32, sf.shape, 0), drafts)
        ok = lax.broadcasted_iota(jnp.int32, sf.shape, 1) <= pos
        sf = jnp.where(ok, sf, FLOOR)
        mf = jnp.max(sf, axis=1, keepdims=True)
        pf = jnp.where(ok, jnp.exp(sf - mf), 0.0).astype(BF16)
        tf = jnp.sum(pf.astype(F32), axis=1, keepdims=True)
        of = dot_nn(pf, vf) / tf
        lf = flip(jnp.broadcast_to(mf + jnp.log(tf), (block_rows, 128)))[0:1]

        key_page = lax.div(lax.broadcasted_iota(jnp.int32, (128, tokens), 1), page_tokens)
        row_page = lax.broadcasted_iota(jnp.int32, (128, tokens), 0)
        ex[...] = (key_page == row_page).astype(F32).astype(BF16)

        wait_bytes(idbr, nb - 1, b_recv)
        joined = idbr[0]
        for i in range(1, nb):
            joined = joined + idbr[i]
        idas[...] = joined
        idar[a] = joined
        send(a_dev, order_a, lambda t: idas, idar, a, a_send, a_recv)
        wait_bytes(vs, heads, v_sem)
        wait_bytes(idar, na - 1, a_recv)

        local = rows_of(idar, na) - ((z * nx + x) * nc + c) * pages
        counts = [
            jnp.sum((local == p).astype(F32), axis=0, keepdims=True) for p in range(pages)
        ]
        counts.append(jnp.zeros((128 - pages, 128), F32))
        counts = jnp.concatenate(counts, axis=0).astype(BF16)
        lane_head = lax.rem(lax.broadcasted_iota(jnp.int32, (heads, 128), 1), heads)
        pick = (lane_head == lax.broadcasted_iota(jnp.int32, (heads, 128), 0)).astype(F32).astype(BF16)
        picked = dot_nt(pick, counts).astype(BF16)
        usable = dot_nn(picked, ex[...])

        lanes = lax.broadcasted_iota(jnp.int32, (block_rows, 128), 1)
        stats = jnp.zeros((block_rows, 128), F32)
        for h in range(heads):
            s = jnp.where(usable[h : h + 1] > 0.5, s_ref[h], FLOOR)
            top = jnp.max(s, axis=1, keepdims=True)
            offset = jnp.where(top > 0.5 * FLOOR, top, 0.0)
            p = jnp.exp(s - offset).astype(BF16)
            total = jnp.sum(p.astype(F32), axis=1, keepdims=True)
            safe = jnp.maximum(total, 0.5)
            o = dot_nn(p, vs[h]) / safe
            lse = jnp.where(total > 0.0, offset + jnp.log(safe), FLOOR)
            for i in range(per_head):
                part = slice(i * block_rows, (i + 1) * block_rows)
                o1s[h * per_head + i] = o[part].astype(BF16)
                stats = jnp.where(lanes == h * per_head + i, lse[part], stats)
        stats = flip(stats)
        for i in range(na):
            l1s[i] = stats[i : i + 1]
        l1r[a] = l1s[a]
        send(a_dev, order_a, lambda t: l1s.at[t], l1r, a, l1_send, l1_recv)
        send(a_dev, order_a, lambda t: o1s.at[t], o1r, a, o1_send, o1_recv)
        o1r[a] = o1s[a]
        wait_bytes(l1r, na - 1, l1_recv)
        w, lse = merge_weights(rows_of(l1r, na))
        w = flip(w)[0:block_rows]
        l2s[...] = lse
        l2r[b] = lse
        send_pairs(range(nb), l2s, l2r, l2_send, l2_recv)
        wait_bytes(o1r, na - 1, o1_recv)
        o = w[:, 0:1] * o1r[0].astype(F32)
        for i in range(1, na):
            o = o + w[:, i : i + 1] * o1r[i].astype(F32)
        o = o.astype(BF16)
        o2s[...] = o
        o2r[b] = o
        send_pairs(range(nb // 4), o2s, o2r, o2_send, o2_recv)
        wait_bytes(l2r, nb - 1, l2_recv)
        send_pairs(range(nb // 4, nb), o2s, o2r, o2_send, o2_recv)
        w, _ = merge_weights(jnp.concatenate([lf, rows_of(l2r, nb)], axis=0))
        w = flip(w)[0:block_rows]
        o = w[:, 0:1] * of
        wait_bytes(o2r, nb - 1, o2_recv)
        for i in range(nb):
            o = o + w[:, i + 1 : i + 2] * o2r[i].astype(F32)
        o = o.astype(BF16)
        block = jnp.concatenate(
            [o[i * drafts : (i + 1) * drafts] for i in range(width // 128)], axis=1
        )
        fs[...] = block
        fr[a] = block
        send(a_dev, order_a, lambda t: fs, fr, a, f_send, f_recv)
        wait_bytes(fr, na - 1, f_recv)
        for i in range(na):
            out_ref[:, i * width : (i + 1) * width] = fr[i]
        wait_bytes(idbr, nb - 1, b_send)
        wait_bytes(idar, na - 1, a_send)
        wait_bytes(o1r, na - 1, o1_send)
        wait_bytes(l1r, na - 1, l1_send)
        wait_bytes(o2r, nb - 1, o2_send)
        wait_bytes(l2r, nb - 1, l2_send)
        wait_bytes(fr, na - 1, f_send)

    dma = pltpu.SemaphoreType.DMA
    span = heads * 128
    rows = heads * groups * drafts // heads
    scratch = [
        pltpu.VMEM((drafts, heads * groups * 128), BF16),
        pltpu.VMEM((128 // nb // heads, heads), jnp.int32),
        pltpu.VMEM((drafts, span), BF16),
        pltpu.VMEM((drafts, span), BF16),
        dma((4,)),
        pltpu.VMEM((heads, tokens, 128), BF16),
        pltpu.VMEM((heads, tokens, 128), BF16),
        pltpu.VMEM((heads, rows, tokens), F32),
        pltpu.VMEM((1, 128), jnp.int32),
        pltpu.VMEM((nb, 1, 128), jnp.int32),
        pltpu.VMEM((1, 128), jnp.int32),
        pltpu.VMEM((na, 1, 128), jnp.int32),
        pltpu.VMEM((na, block_rows, 128), BF16),
        pltpu.VMEM((na, 1, 128), F32),
        pltpu.VMEM((na, block_rows, 128), BF16),
        pltpu.VMEM((na, 1, 128), F32),
        pltpu.VMEM((block_rows, 128), BF16),
        pltpu.VMEM((1, 128), F32),
        pltpu.VMEM((nb, block_rows, 128), BF16),
        pltpu.VMEM((nb, 1, 128), F32),
        pltpu.VMEM((drafts, width), BF16),
        pltpu.VMEM((na, drafts, width), BF16),
        pltpu.VMEM((128, tokens), BF16),
        *[dma] * 16,
    ]
    vmem = pl.BlockSpec(memory_space=pltpu.VMEM)
    hbm = pl.BlockSpec(memory_space=pltpu.HBM)
    return pl.pallas_call(
        kernel,
        out_shape=jax.ShapeDtypeStruct((drafts, heads * groups * 128), BF16),
        in_specs=[hbm] * 6,
        out_specs=vmem,
        scratch_shapes=scratch,
        compiler_params=pltpu.CompilerParams(
            collective_id=0, has_side_effects=True, vmem_limit_bytes=32 * 1024 * 1024
        ),
    )


def solution(mesh):
    nz, nx, nc = 16, 4, 2
    torus = Mesh(
        mesh.devices.reshape(mesh.shape["grp"], nz, nx, nc), ("grp", "page_0", "page_1", "page_2")
    )

    def on_device(queries, key_cache, value_cache, new_keys, new_values, chosen):
        pages, page_tokens, span = key_cache.shape
        heads = chosen.shape[0]
        drafts = queries.shape[0]
        groups = queries.shape[1] // span
        call = make_kernel(
            nz, nx, nc, heads, pages * page_tokens, page_tokens, drafts, groups,
            (span // heads) ** (-0.5),
        )
        return call(
            *[
                pltpu.with_memory_space_constraint(x, pltpu.HBM)
                for x in (
                    queries, chosen.T, new_keys, new_values,
                    key_cache.reshape(-1, span), value_cache.reshape(-1, span),
                )
            ]
        )

    in_specs = (
        P("grp", None),
        P(GRP_PAGE, None, None),
        P(GRP_PAGE, None, None),
        P("grp", None),
        P("grp", None),
        P("grp", PAGE),
    )
    return jax.shard_map(
        on_device, mesh=torus, in_specs=in_specs, out_specs=P("grp", None), check_vma=False
    )
```

```python
import jax
import jax.numpy as jnp
from jax import lax
from jax.experimental import pallas as pl
from jax.experimental.pallas import tpu as pltpu
from jax.sharding import Mesh
from jax.sharding import PartitionSpec as P

GRP_PAGE = ("grp", "page_0", "page_1", "page_2")
PAGE = GRP_PAGE[1:]
FLOOR = -1e30
F32 = jnp.float32
BF16 = jnp.bfloat16
MESH = pl.DeviceIdType.MESH


def dot_nt(a, b):
    return lax.dot_general(a, b, (((1,), (1,)), ((), ())), preferred_element_type=F32)


def dot_nn(a, b):
    return lax.dot_general(a, b, (((1,), (0,)), ((), ())), preferred_element_type=F32)


def rows_of(ref, count):
    return jnp.concatenate([ref[i] for i in range(count)], axis=0)


def flip(x):
    n = x.shape[0]
    if n < 128:
        x = jnp.concatenate([x, jnp.zeros((128 - n, 128), x.dtype)], axis=0)
    return jnp.transpose(x)


def merge_weights(lse):
    top = jnp.max(lse, axis=0, keepdims=True)
    w = jnp.exp(lse - top)
    total = jnp.sum(w, axis=0, keepdims=True)
    return w / total, top + jnp.log(total)


def far_first(n, ring):
    def key(d):
        return -min(d // ring, (n - d) // ring)

    return sorted(range(1, n), key=key)


def make_kernel(nz, nx, nc, heads, tokens, page_tokens, drafts, groups, scaling):
    na = nx * nc * 2
    nb = nz // 2
    pages = tokens // page_tokens
    block_rows = heads * groups * drafts // na
    per_head = na // heads
    halves = block_rows // drafts
    width = halves * 128

    def kernel(
        q_hbm, ids_hbm, nk_hbm, nv_hbm, k_hbm, v_hbm, out_ref,
        q_ref, ids_ref, nk_ref, nv_ref, small_sem, ks, vs, s_ref, idbs, idbr, idas, idar,
        o1s, l1s, o1r, l1r, o2s, l2s, o2r, l2r, fs, fr, ex,
        k_sem, v_sem, b_send, b_recv, a_send, a_recv,
        o1_send, o1_recv, l1_send, l1_recv,
        o2_send, o2_recv, l2_send, l2_recv, f_send, f_recv,
    ):
        z = lax.axis_index("page_0")
        x = lax.axis_index("page_1")
        c = lax.axis_index("page_2")
        zlow = lax.rem(z, 2)
        b = lax.div(z, 2)
        a = (x * nc + c) * 2 + zlow

        def a_dev(d):
            t = lax.rem(a + d, na)
            u = lax.div(t, 2)
            return t, {
                "page_0": b * 2 + lax.rem(t, 2),
                "page_1": lax.div(u, nc),
                "page_2": lax.rem(u, nc),
            }

        def b_dev(d):
            t = lax.rem(b + d, nb)
            return t, {"page_0": t * 2 + zlow, "page_1": x, "page_2": c}

        order_a = far_first(na, nc * 2)
        order_b = far_first(nb, 1)

        def copy(src, dst, ss, rs, dev):
            return pltpu.make_async_remote_copy(
                src_ref=src, dst_ref=dst, send_sem=ss, recv_sem=rs,
                device_id=dev, device_id_type=MESH,
            )

        def send(group, order, src, dst, me, ss, rs):
            for d in order:
                t, dev = group(d)
                copy(src(t), dst.at[me], ss, rs, dev).start()

        def wait_bytes(buf, count, sem):
            part = buf.at[pl.ds(0, count)]
            pltpu.make_async_copy(part, part, sem).wait()

        small = [
            pltpu.make_async_copy(src, dst, small_sem.at[i])
            for i, (src, dst) in enumerate(
                [(ids_hbm, ids_ref), (q_hbm, q_ref), (nk_hbm, nk_ref), (nv_hbm, nv_ref)]
            )
        ]
        small[0].start()

        def send_pairs(src, dst, ss, rs):
            for t in range(nb):
                d = lax.rem(t - b + nb, nb)

                @pl.when(d != 0)
                def _():
                    copy(src, dst.at[b], ss, rs, b_dev(d)[1]).start()

        barrier = pltpu.get_barrier_semaphore()
        for d in order_b:
            pl.semaphore_signal(barrier, inc=1, device_id=b_dev(d)[1], device_id_type=MESH)
        for d in order_a:
            pl.semaphore_signal(barrier, inc=1, device_id=a_dev(d)[1], device_id_type=MESH)

        def load(src, dst, sem, h):
            return pltpu.make_async_copy(src.at[:, pl.ds(h * 128, 128)], dst.at[h], sem)

        for r in small[1:]:
            r.start()
        for h in range(heads):
            load(k_hbm, ks, k_sem, h).start()
        for h in range(heads):
            load(v_hbm, vs, v_sem, h).start()

        lane = lax.broadcasted_iota(jnp.int32, (1, 128), 1)
        slot = 128 // nb
        small[0].wait()
        ids = ids_ref[...]
        ids = jnp.concatenate([ids[j : j + 1] for j in range(ids.shape[0])] * nb, axis=1)
        idbs[...] = jnp.where(lax.div(lane, slot) == b, ids, 0)
        idbr[b] = idbs[...]

        def scores(h):
            base = h * groups * 128
            q = jnp.concatenate(
                [q_ref[:, base + g * 128 : base + (g + 1) * 128] for g in range(groups)], axis=0
            )
            s_ref[h] = dot_nt(q, ks[h]) * scaling

        pl.semaphore_wait(barrier, na - 1 + nb - 1)
        send(b_dev, order_b, lambda t: idbs, idbr, b, b_send, b_recv)
        for r in small[1:]:
            r.wait()
        wait_bytes(ks, heads, k_sem)
        for h in range(heads):
            scores(h)

        cols = pl.multiple_of(a * width, width)
        head_cols = pl.multiple_of(lax.div(a, per_head) * 128, 128)
        q_own = q_ref[:, pl.ds(cols, width)]
        q_own = jnp.concatenate(
            [q_own[:, i * 128 : (i + 1) * 128] for i in range(width // 128)], axis=0
        )
        pad = jnp.zeros((128 - drafts, 128), BF16)
        kf = jnp.concatenate([nk_ref[:, pl.ds(head_cols, 128)], pad], axis=0)
        vf = jnp.concatenate([nv_ref[:, pl.ds(head_cols, 128)], pad], axis=0)
        sf = dot_nt(q_own, kf) * scaling
        pos = lax.rem(lax.broadcasted_iota(jnp.int32, sf.shape, 0), drafts)
        ok = lax.broadcasted_iota(jnp.int32, sf.shape, 1) <= pos
        sf = jnp.where(ok, sf, FLOOR)
        mf = jnp.max(sf, axis=1, keepdims=True)
        pf = jnp.where(ok, jnp.exp(sf - mf), 0.0).astype(BF16)
        tf = jnp.sum(pf.astype(F32), axis=1, keepdims=True)
        of = dot_nn(pf, vf) / tf
        lf = flip(jnp.broadcast_to(mf + jnp.log(tf), (block_rows, 128)))[0:1]

        key_page = lax.div(lax.broadcasted_iota(jnp.int32, (128, tokens), 1), page_tokens)
        row_page = lax.broadcasted_iota(jnp.int32, (128, tokens), 0)
        ex[...] = (key_page == row_page).astype(F32).astype(BF16)

        wait_bytes(idbr, nb - 1, b_recv)
        joined = idbr[0]
        for i in range(1, nb):
            joined = joined + idbr[i]
        idas[...] = joined
        idar[a] = joined
        send(a_dev, order_a, lambda t: idas, idar, a, a_send, a_recv)
        wait_bytes(vs, heads, v_sem)
        wait_bytes(idar, na - 1, a_recv)

        local = rows_of(idar, na) - ((z * nx + x) * nc + c) * pages
        counts = [
            jnp.sum((local == p).astype(F32), axis=0, keepdims=True) for p in range(pages)
        ]
        counts.append(jnp.zeros((128 - pages, 128), F32))
        counts = jnp.concatenate(counts, axis=0).astype(BF16)
        lane_head = lax.rem(lax.broadcasted_iota(jnp.int32, (heads, 128), 1), heads)
        pick = (lane_head == lax.broadcasted_iota(jnp.int32, (heads, 128), 0)).astype(F32).astype(BF16)
        picked = dot_nt(pick, counts).astype(BF16)
        usable = dot_nn(picked, ex[...])

        lanes = lax.broadcasted_iota(jnp.int32, (block_rows, 128), 1)
        stats = jnp.zeros((block_rows, 128), F32)
        for h in range(heads):
            s = jnp.where(usable[h : h + 1] > 0.5, s_ref[h], FLOOR)
            top = jnp.max(s, axis=1, keepdims=True)
            offset = jnp.where(top > 0.5 * FLOOR, top, 0.0)
            p = jnp.exp(s - offset).astype(BF16)
            total = jnp.sum(p.astype(F32), axis=1, keepdims=True)
            safe = jnp.maximum(total, 0.5)
            o = dot_nn(p, vs[h]) / safe
            lse = jnp.where(total > 0.0, offset + jnp.log(safe), FLOOR)
            for i in range(per_head):
                part = slice(i * block_rows, (i + 1) * block_rows)
                o1s[h * per_head + i] = o[part].astype(BF16)
                stats = jnp.where(lanes == h * per_head + i, lse[part], stats)
        stats = flip(stats)
        for i in range(na):
            l1s[i] = stats[i : i + 1]
        l1r[a] = l1s[a]
        send(a_dev, order_a, lambda t: l1s.at[t], l1r, a, l1_send, l1_recv)
        send(a_dev, order_a, lambda t: o1s.at[t], o1r, a, o1_send, o1_recv)
        o1r[a] = o1s[a]
        wait_bytes(l1r, na - 1, l1_recv)
        w, lse = merge_weights(rows_of(l1r, na))
        w = flip(w)[0:block_rows]
        l2s[...] = lse
        l2r[b] = lse
        send_pairs(l2s, l2r, l2_send, l2_recv)
        wait_bytes(o1r, na - 1, o1_recv)
        for k in range(halves):
            part = slice(k * drafts, (k + 1) * drafts)
            o = w[part, 0:1] * o1r[0, part].astype(F32)
            for i in range(1, na):
                o = o + w[part, i : i + 1] * o1r[i, part].astype(F32)
            o = o.astype(BF16)
            o2s[k] = o
            o2r[k, b] = o
            send_pairs(o2s.at[k], o2r.at[k], o2_send.at[k], o2_recv.at[k])
        wait_bytes(l2r, nb - 1, l2_recv)
        w, _ = merge_weights(jnp.concatenate([lf, rows_of(l2r, nb)], axis=0))
        w = flip(w)[0:block_rows]
        for k in range(halves):
            part = slice(k * drafts, (k + 1) * drafts)
            o = w[part, 0:1] * of[part]
            wait_bytes(o2r.at[k], nb - 1, o2_recv.at[k])
            for i in range(nb):
                o = o + w[part, i + 1 : i + 2] * o2r[k, i].astype(F32)
            o = o.astype(BF16)
            fs[k] = o
            fr[k, a] = o
            send(a_dev, order_a, lambda t: fs.at[k], fr.at[k], a, f_send.at[k], f_recv.at[k])
        for k in range(halves):
            wait_bytes(fr.at[k], na - 1, f_recv.at[k])
            for i in range(na):
                at = i * width + k * 128
                out_ref[:, at : at + 128] = fr[k, i]
        wait_bytes(idbr, nb - 1, b_send)
        wait_bytes(idar, na - 1, a_send)
        wait_bytes(o1r, na - 1, o1_send)
        wait_bytes(l1r, na - 1, l1_send)
        wait_bytes(l2r, nb - 1, l2_send)
        for k in range(halves):
            wait_bytes(o2r.at[k], nb - 1, o2_send.at[k])
            wait_bytes(fr.at[k], na - 1, f_send.at[k])

    dma = pltpu.SemaphoreType.DMA
    span = heads * 128
    rows = heads * groups * drafts // heads
    scratch = [
        pltpu.VMEM((drafts, heads * groups * 128), BF16),
        pltpu.VMEM((128 // nb // heads, heads), jnp.int32),
        pltpu.VMEM((drafts, span), BF16),
        pltpu.VMEM((drafts, span), BF16),
        dma((4,)),
        pltpu.VMEM((heads, tokens, 128), BF16),
        pltpu.VMEM((heads, tokens, 128), BF16),
        pltpu.VMEM((heads, rows, tokens), F32),
        pltpu.VMEM((1, 128), jnp.int32),
        pltpu.VMEM((nb, 1, 128), jnp.int32),
        pltpu.VMEM((1, 128), jnp.int32),
        pltpu.VMEM((na, 1, 128), jnp.int32),
        pltpu.VMEM((na, block_rows, 128), BF16),
        pltpu.VMEM((na, 1, 128), F32),
        pltpu.VMEM((na, block_rows, 128), BF16),
        pltpu.VMEM((na, 1, 128), F32),
        pltpu.VMEM((halves, drafts, 128), BF16),
        pltpu.VMEM((1, 128), F32),
        pltpu.VMEM((halves, nb, drafts, 128), BF16),
        pltpu.VMEM((nb, 1, 128), F32),
        pltpu.VMEM((halves, drafts, 128), BF16),
        pltpu.VMEM((halves, na, drafts, 128), BF16),
        pltpu.VMEM((128, tokens), BF16),
        *[dma] * 10, *[dma((halves,))] * 2, *[dma] * 2, *[dma((halves,))] * 2,
    ]
    vmem = pl.BlockSpec(memory_space=pltpu.VMEM)
    hbm = pl.BlockSpec(memory_space=pltpu.HBM)
    return pl.pallas_call(
        kernel,
        out_shape=jax.ShapeDtypeStruct((drafts, heads * groups * 128), BF16),
        in_specs=[hbm] * 6,
        out_specs=vmem,
        scratch_shapes=scratch,
        compiler_params=pltpu.CompilerParams(
            collective_id=0, has_side_effects=True, vmem_limit_bytes=32 * 1024 * 1024
        ),
    )


def solution(mesh):
    nz, nx, nc = 16, 4, 2
    torus = Mesh(
        mesh.devices.reshape(mesh.shape["grp"], nz, nx, nc), ("grp", "page_0", "page_1", "page_2")
    )

    def on_device(queries, key_cache, value_cache, new_keys, new_values, chosen):
        pages, page_tokens, span = key_cache.shape
        heads = chosen.shape[0]
        drafts = queries.shape[0]
        groups = queries.shape[1] // span
        call = make_kernel(
            nz, nx, nc, heads, pages * page_tokens, page_tokens, drafts, groups,
            (span // heads) ** (-0.5),
        )
        return call(
            *[
                pltpu.with_memory_space_constraint(x, pltpu.HBM)
                for x in (
                    queries, chosen.T, new_keys, new_values,
                    key_cache.reshape(-1, span), value_cache.reshape(-1, span),
                )
            ]
        )

    in_specs = (
        P("grp", None),
        P(GRP_PAGE, None, None),
        P(GRP_PAGE, None, None),
        P("grp", None),
        P("grp", None),
        P("grp", PAGE),
    )
    return jax.shard_map(
        on_device, mesh=torus, in_specs=in_specs, out_specs=P("grp", None), check_vma=False
    )
```

```python
import jax
import jax.numpy as jnp
from jax import lax
from jax.experimental import pallas as pl
from jax.experimental.pallas import tpu as pltpu
from jax.sharding import Mesh
from jax.sharding import PartitionSpec as P

GRP_PAGE = ("grp", "page_0", "page_1", "page_2")
PAGE = GRP_PAGE[1:]
FLOOR = -1e30
F32 = jnp.float32
BF16 = jnp.bfloat16
MESH = pl.DeviceIdType.MESH


def dot_nt(a, b):
    return lax.dot_general(a, b, (((1,), (1,)), ((), ())), preferred_element_type=F32)


def dot_nn(a, b):
    return lax.dot_general(a, b, (((1,), (0,)), ((), ())), preferred_element_type=F32)


def rows_of(ref, count):
    return jnp.concatenate([ref[i] for i in range(count)], axis=0)


def flip(x):
    n = x.shape[0]
    if n < 128:
        x = jnp.concatenate([x, jnp.zeros((128 - n, 128), x.dtype)], axis=0)
    return jnp.transpose(x)


def merge_weights(lse):
    top = jnp.max(lse, axis=0, keepdims=True)
    w = jnp.exp(lse - top)
    total = jnp.sum(w, axis=0, keepdims=True)
    return w / total, top + jnp.log(total)


def far_first(n, ring):
    def key(d):
        return -min(d // ring, (n - d) // ring)

    return sorted(range(1, n), key=key)


def make_kernel(nz, nx, nc, heads, ids_each, tokens, page_tokens, drafts, groups, scaling):
    na = nx * nc * 2
    nb = nz // 2
    pages = tokens // page_tokens
    id_rows = nz * ids_each // 128
    block_rows = heads * groups * drafts // na
    per_head = na // heads
    width = block_rows // drafts * 128

    def kernel(
        q_hbm, ids_hbm, nk_hbm, nv_hbm, k_hbm, v_hbm, out_ref,
        q_ref, ids_ref, nk_ref, nv_ref, small_sem, ks, vs, s_ref, idbs, idbr, idas, idar,
        o1s, l1s, o1r, l1r, o2s, l2s, o2r, l2r, fs, fr, ex,
        k_sem, v_sem, b_send, b_recv, a_send, a_recv,
        o1_send, o1_recv, l1_send, l1_recv,
        o2_send, o2_recv, l2_send, l2_recv, f_send, f_recv,
    ):
        z = lax.axis_index("page_0")
        x = lax.axis_index("page_1")
        c = lax.axis_index("page_2")
        zlow = lax.rem(z, 2)
        b = lax.div(z, 2)
        a = (x * nc + c) * 2 + zlow

        def a_dev(d):
            t = lax.rem(a + d, na)
            u = lax.div(t, 2)
            return t, {
                "page_0": b * 2 + lax.rem(t, 2),
                "page_1": lax.div(u, nc),
                "page_2": lax.rem(u, nc),
            }

        def b_dev(d):
            t = lax.rem(b + d, nb)
            return t, {"page_0": t * 2 + zlow, "page_1": x, "page_2": c}

        def z_dev(d):
            t = lax.rem(z + d, nz)
            return t, {"page_0": t, "page_1": x, "page_2": c}

        def plane_dev(d):
            t = lax.rem(x * nc + c + d, nx * nc)
            return t, {"page_0": z, "page_1": lax.div(t, nc), "page_2": lax.rem(t, nc)}

        order_z = far_first(nz, 1)
        order_plane = far_first(nx * nc, nc)
        order_a = far_first(na, nc * 2)
        order_b = far_first(nb, 1)

        def copy(src, dst, ss, rs, dev):
            return pltpu.make_async_remote_copy(
                src_ref=src, dst_ref=dst, send_sem=ss, recv_sem=rs,
                device_id=dev, device_id_type=MESH,
            )

        def send(group, order, src, dst, me, ss, rs):
            for d in order:
                t, dev = group(d)
                copy(src(t), dst.at[me], ss, rs, dev).start()

        def wait_bytes(buf, count, sem):
            part = buf.at[pl.ds(0, count)]
            pltpu.make_async_copy(part, part, sem).wait()

        small = [
            pltpu.make_async_copy(src, dst, small_sem.at[i])
            for i, (src, dst) in enumerate(
                [(ids_hbm, ids_ref), (q_hbm, q_ref), (nk_hbm, nk_ref), (nv_hbm, nv_ref)]
            )
        ]
        small[0].start()

        def send_pairs(src, dst, ss, rs):
            for t in range(nb):
                d = lax.rem(t - b + nb, nb)

                @pl.when(d != 0)
                def _():
                    copy(src, dst.at[b], ss, rs, b_dev(d)[1]).start()

        barrier = pltpu.get_barrier_semaphore()
        for d in order_z:
            pl.semaphore_signal(barrier, inc=1, device_id=z_dev(d)[1], device_id_type=MESH)
        for d in order_a:
            pl.semaphore_signal(barrier, inc=1, device_id=a_dev(d)[1], device_id_type=MESH)

        def load(src, dst, sem, h):
            return pltpu.make_async_copy(src.at[:, pl.ds(h * 128, 128)], dst.at[h], sem)

        for r in small[1:]:
            r.start()
        for h in range(heads):
            load(k_hbm, ks, k_sem, h).start()
        for h in range(heads):
            load(v_hbm, vs, v_sem, h).start()

        lane = lax.broadcasted_iota(jnp.int32, (1, 128), 1)
        slots = nz // id_rows
        slot = 128 // slots
        small[0].wait()
        ids = ids_ref[...]
        ids = jnp.concatenate([ids[j : j + 1] for j in range(ids.shape[0])] * slots, axis=1)
        idbs[...] = jnp.where(lax.div(lane, slot) == lax.rem(z, slots), ids, 0)
        idbr[z] = idbs[...]

        def scores(h):
            base = h * groups * 128
            q = jnp.concatenate(
                [q_ref[:, base + g * 128 : base + (g + 1) * 128] for g in range(groups)], axis=0
            )
            s_ref[h] = dot_nt(q, ks[h]) * scaling

        pl.semaphore_wait(barrier, na - 1 + nz - 1)
        send(z_dev, order_z, lambda t: idbs, idbr, z, b_send, b_recv)
        for r in small[1:]:
            r.wait()
        wait_bytes(ks, heads, k_sem)
        for h in range(heads):
            scores(h)

        cols = pl.multiple_of(a * width, width)
        head_cols = pl.multiple_of(lax.div(a, per_head) * 128, 128)
        q_own = q_ref[:, pl.ds(cols, width)]
        q_own = jnp.concatenate(
            [q_own[:, i * 128 : (i + 1) * 128] for i in range(width // 128)], axis=0
        )
        pad = jnp.zeros((128 - drafts, 128), BF16)
        kf = jnp.concatenate([nk_ref[:, pl.ds(head_cols, 128)], pad], axis=0)
        vf = jnp.concatenate([nv_ref[:, pl.ds(head_cols, 128)], pad], axis=0)
        sf = dot_nt(q_own, kf) * scaling
        pos = lax.rem(lax.broadcasted_iota(jnp.int32, sf.shape, 0), drafts)
        ok = lax.broadcasted_iota(jnp.int32, sf.shape, 1) <= pos
        sf = jnp.where(ok, sf, FLOOR)
        mf = jnp.max(sf, axis=1, keepdims=True)
        pf = jnp.where(ok, jnp.exp(sf - mf), 0.0).astype(BF16)
        tf = jnp.sum(pf.astype(F32), axis=1, keepdims=True)
        of = dot_nn(pf, vf) / tf
        lf = flip(jnp.broadcast_to(mf + jnp.log(tf), (block_rows, 128)))[0:1]

        key_page = lax.div(lax.broadcasted_iota(jnp.int32, (128, tokens), 1), page_tokens)
        row_page = lax.broadcasted_iota(jnp.int32, (128, tokens), 0)
        ex[...] = (key_page == row_page).astype(F32).astype(BF16)

        wait_bytes(idbr, nz - 1, b_recv)
        for r in range(id_rows):
            joined = idbr[r * slots]
            for i in range(r * slots + 1, (r + 1) * slots):
                joined = joined + idbr[i]
            idas[r] = joined
            idar[x * nc + c, r] = joined
        send(plane_dev, order_plane, lambda t: idas, idar, x * nc + c, a_send, a_recv)
        wait_bytes(vs, heads, v_sem)
        wait_bytes(idar, nx * nc - 1, a_recv)

        local = jnp.concatenate(
            [idar[i, r] for i in range(nx * nc) for r in range(id_rows)], axis=0
        )
        local = local - ((z * nx + x) * nc + c) * pages
        counts = [
            jnp.sum((local == p).astype(F32), axis=0, keepdims=True) for p in range(pages)
        ]
        counts.append(jnp.zeros((128 - pages, 128), F32))
        counts = jnp.concatenate(counts, axis=0).astype(BF16)
        lane_head = lax.rem(lax.broadcasted_iota(jnp.int32, (heads, 128), 1), heads)
        pick = (lane_head == lax.broadcasted_iota(jnp.int32, (heads, 128), 0)).astype(F32).astype(BF16)
        picked = dot_nt(pick, counts).astype(BF16)
        usable = dot_nn(picked, ex[...])

        lanes = lax.broadcasted_iota(jnp.int32, (block_rows, 128), 1)
        stats = jnp.zeros((block_rows, 128), F32)
        for h in range(heads):
            s = jnp.where(usable[h : h + 1] > 0.5, s_ref[h], FLOOR)
            top = jnp.max(s, axis=1, keepdims=True)
            offset = jnp.where(top > 0.5 * FLOOR, top, 0.0)
            p = jnp.exp(s - offset).astype(BF16)
            total = jnp.sum(p.astype(F32), axis=1, keepdims=True)
            safe = jnp.maximum(total, 0.5)
            o = dot_nn(p, vs[h]) / safe
            lse = jnp.where(total > 0.0, offset + jnp.log(safe), FLOOR)
            for i in range(per_head):
                part = slice(i * block_rows, (i + 1) * block_rows)
                o1s[h * per_head + i] = o[part].astype(BF16)
                stats = jnp.where(lanes == h * per_head + i, lse[part], stats)
        stats = flip(stats)
        for i in range(na):
            l1s[i] = stats[i : i + 1]
        l1r[a] = l1s[a]
        send(a_dev, order_a, lambda t: l1s.at[t], l1r, a, l1_send, l1_recv)
        send(a_dev, order_a, lambda t: o1s.at[t], o1r, a, o1_send, o1_recv)
        o1r[a] = o1s[a]
        wait_bytes(l1r, na - 1, l1_recv)
        w, lse = merge_weights(rows_of(l1r, na))
        w = flip(w)[0:block_rows]
        l2s[...] = lse
        l2r[b] = lse
        send_pairs(l2s, l2r, l2_send, l2_recv)
        wait_bytes(o1r, na - 1, o1_recv)
        o = w[:, 0:1] * o1r[0].astype(F32)
        for i in range(1, na):
            o = o + w[:, i : i + 1] * o1r[i].astype(F32)
        o = o.astype(BF16)
        o2s[...] = o
        o2r[b] = o
        send_pairs(o2s, o2r, o2_send, o2_recv)
        wait_bytes(l2r, nb - 1, l2_recv)
        w, _ = merge_weights(jnp.concatenate([lf, rows_of(l2r, nb)], axis=0))
        w = flip(w)[0:block_rows]
        o = w[:, 0:1] * of
        wait_bytes(o2r, nb - 1, o2_recv)
        for i in range(nb):
            o = o + w[:, i + 1 : i + 2] * o2r[i].astype(F32)
        o = o.astype(BF16)
        block = jnp.concatenate(
            [o[i * drafts : (i + 1) * drafts] for i in range(width // 128)], axis=1
        )
        fs[...] = block
        fr[a] = block
        send(a_dev, order_a, lambda t: fs, fr, a, f_send, f_recv)
        wait_bytes(fr, na - 1, f_recv)
        for i in range(na):
            out_ref[:, i * width : (i + 1) * width] = fr[i]
        wait_bytes(idbr, nz - 1, b_send)
        wait_bytes(idar, nx * nc - 1, a_send)
        wait_bytes(o1r, na - 1, o1_send)
        wait_bytes(l1r, na - 1, l1_send)
        wait_bytes(o2r, nb - 1, o2_send)
        wait_bytes(l2r, nb - 1, l2_send)
        wait_bytes(fr, na - 1, f_send)

    dma = pltpu.SemaphoreType.DMA
    span = heads * 128
    rows = heads * groups * drafts // heads
    scratch = [
        pltpu.VMEM((drafts, heads * groups * 128), BF16),
        pltpu.VMEM((ids_each // heads, heads), jnp.int32),
        pltpu.VMEM((drafts, span), BF16),
        pltpu.VMEM((drafts, span), BF16),
        dma((4,)),
        pltpu.VMEM((heads, tokens, 128), BF16),
        pltpu.VMEM((heads, tokens, 128), BF16),
        pltpu.VMEM((heads, rows, tokens), F32),
        pltpu.VMEM((1, 128), jnp.int32),
        pltpu.VMEM((nz, 1, 128), jnp.int32),
        pltpu.VMEM((id_rows, 1, 128), jnp.int32),
        pltpu.VMEM((nx * nc, id_rows, 1, 128), jnp.int32),
        pltpu.VMEM((na, block_rows, 128), BF16),
        pltpu.VMEM((na, 1, 128), F32),
        pltpu.VMEM((na, block_rows, 128), BF16),
        pltpu.VMEM((na, 1, 128), F32),
        pltpu.VMEM((block_rows, 128), BF16),
        pltpu.VMEM((1, 128), F32),
        pltpu.VMEM((nb, block_rows, 128), BF16),
        pltpu.VMEM((nb, 1, 128), F32),
        pltpu.VMEM((drafts, width), BF16),
        pltpu.VMEM((na, drafts, width), BF16),
        pltpu.VMEM((128, tokens), BF16),
        *[dma] * 16,
    ]
    vmem = pl.BlockSpec(memory_space=pltpu.VMEM)
    hbm = pl.BlockSpec(memory_space=pltpu.HBM)
    return pl.pallas_call(
        kernel,
        out_shape=jax.ShapeDtypeStruct((drafts, heads * groups * 128), BF16),
        in_specs=[hbm] * 6,
        out_specs=vmem,
        scratch_shapes=scratch,
        compiler_params=pltpu.CompilerParams(
            collective_id=0, has_side_effects=True, vmem_limit_bytes=32 * 1024 * 1024
        ),
    )


def solution(mesh):
    nz, nx, nc = 16, 4, 2
    torus = Mesh(
        mesh.devices.reshape(mesh.shape["grp"], nz, nx, nc), ("grp", "page_0", "page_1", "page_2")
    )

    def on_device(queries, key_cache, value_cache, new_keys, new_values, chosen):
        pages, page_tokens, span = key_cache.shape
        heads = chosen.shape[0]
        drafts = queries.shape[0]
        groups = queries.shape[1] // span
        call = make_kernel(
            nz, nx, nc, heads, chosen.size, pages * page_tokens, page_tokens, drafts, groups,
            (span // heads) ** (-0.5),
        )
        return call(
            *[
                pltpu.with_memory_space_constraint(x, pltpu.HBM)
                for x in (
                    queries, chosen.T, new_keys, new_values,
                    key_cache.reshape(-1, span), value_cache.reshape(-1, span),
                )
            ]
        )

    in_specs = (
        P("grp", None),
        P(GRP_PAGE, None, None),
        P(GRP_PAGE, None, None),
        P("grp", None),
        P("grp", None),
        P("grp", PAGE),
    )
    return jax.shard_map(
        on_device, mesh=torus, in_specs=in_specs, out_specs=P("grp", None), check_vma=False
    )
```

```python
import jax
import jax.numpy as jnp
from jax import lax
from jax.experimental import pallas as pl
from jax.experimental.pallas import tpu as pltpu
from jax.sharding import Mesh
from jax.sharding import PartitionSpec as P

GRP_PAGE = ("grp", "page_0", "page_1", "page_2")
PAGE = GRP_PAGE[1:]
FLOOR = -1e30
F32 = jnp.float32
BF16 = jnp.bfloat16
MESH = pl.DeviceIdType.MESH


def dot_nt(a, b):
    return lax.dot_general(a, b, (((1,), (1,)), ((), ())), preferred_element_type=F32)


def dot_nn(a, b):
    return lax.dot_general(a, b, (((1,), (0,)), ((), ())), preferred_element_type=F32)


def rows_of(ref, count):
    return jnp.concatenate([ref[i] for i in range(count)], axis=0)


def flip(x):
    n = x.shape[0]
    if n < 128:
        x = jnp.concatenate([x, jnp.zeros((128 - n, 128), x.dtype)], axis=0)
    return jnp.transpose(x)


def merge_weights(lse):
    top = jnp.max(lse, axis=0, keepdims=True)
    w = jnp.exp(lse - top)
    total = jnp.sum(w, axis=0, keepdims=True)
    return w / total, top + jnp.log(total)


def far_first(n, ring):
    def key(d):
        return -min(d // ring, (n - d) // ring)

    return sorted(range(1, n), key=key)


def make_kernel(nz, nx, nc, heads, ids_each, tokens, page_tokens, drafts, groups, scaling):
    na = nx * nc * 2
    nb = nz // 2
    pages = tokens // page_tokens
    id_rows = nz * ids_each // 128
    block_rows = heads * groups * drafts // na
    per_head = na // heads
    width = block_rows // drafts * 128

    def kernel(
        q_hbm, ids_hbm, nk_hbm, nv_hbm, k_hbm, v_hbm, out_ref,
        q_ref, ids_ref, nk_ref, nv_ref, small_sem, ks, vs, s_ref, idbs, idbr, idas, idar,
        o1s, l1s, o1r, l1r, o2s, l2s, o2r, l2r, fs, fr, ex,
        k_sem, v_sem, b_send, b_recv, a_send, a_recv,
        o1_send, o1_recv, l1_send, l1_recv,
        o2_send, o2_recv, l2_send, l2_recv, f_send, f_recv,
    ):
        z = lax.axis_index("page_0")
        x = lax.axis_index("page_1")
        c = lax.axis_index("page_2")
        zlow = lax.rem(z, 2)
        b = lax.div(z, 2)
        a = (x * nc + c) * 2 + zlow

        def a_dev(d):
            t = lax.rem(a + d, na)
            u = lax.div(t, 2)
            return t, {
                "page_0": b * 2 + lax.rem(t, 2),
                "page_1": lax.div(u, nc),
                "page_2": lax.rem(u, nc),
            }

        def pair_dev(t):
            return {"page_0": t * 2 + zlow, "page_1": x, "page_2": c}

        def z_dev(d):
            t = lax.rem(z + d, nz)
            return t, {"page_0": t, "page_1": x, "page_2": c}

        def plane_dev(d):
            t = lax.rem(x * nc + c + d, nx * nc)
            return t, {"page_0": z, "page_1": lax.div(t, nc), "page_2": lax.rem(t, nc)}

        order_z = far_first(nz, 1)
        order_plane = far_first(nx * nc, nc)
        order_a = far_first(na, nc * 2)

        def copy(src, dst, ss, rs, dev):
            return pltpu.make_async_remote_copy(
                src_ref=src, dst_ref=dst, send_sem=ss, recv_sem=rs,
                device_id=dev, device_id_type=MESH,
            )

        def send(group, order, src, dst, me, ss, rs):
            for d in order:
                t, dev = group(d)
                copy(src(t), dst.at[me], ss, rs, dev).start()

        def wait_bytes(buf, count, sem):
            part = buf.at[pl.ds(0, count)]
            pltpu.make_async_copy(part, part, sem).wait()

        small = [
            pltpu.make_async_copy(src, dst, small_sem.at[i])
            for i, (src, dst) in enumerate(
                [(ids_hbm, ids_ref), (q_hbm, q_ref), (nk_hbm, nk_ref), (nv_hbm, nv_ref)]
            )
        ]
        small[0].start()

        def after(i, own):
            return i + (i >= own).astype(jnp.int32)

        def send_pairs(src, dst, ss, rs):
            for i in range(nb - 1):
                copy(src, dst.at[b], ss, rs, pair_dev(after(i, b))).start()

        def send_final(src, dst, ss, rs):
            plane = nx * nc
            for i in range(na - 1):
                r = after(i, zlow * plane + x * nc + c)
                u = lax.rem(r, plane)
                dev = {
                    "page_0": b * 2 + lax.div(r, plane),
                    "page_1": lax.div(u, nc),
                    "page_2": lax.rem(u, nc),
                }
                copy(src, dst.at[a], ss, rs, dev).start()

        barrier = pltpu.get_barrier_semaphore()
        for d in order_z:
            pl.semaphore_signal(barrier, inc=1, device_id=z_dev(d)[1], device_id_type=MESH)
        for d in order_a:
            pl.semaphore_signal(barrier, inc=1, device_id=a_dev(d)[1], device_id_type=MESH)

        def load(src, dst, sem, h):
            return pltpu.make_async_copy(src.at[:, pl.ds(h * 128, 128)], dst.at[h], sem)

        for r in small[1:]:
            r.start()
        for h in range(heads):
            load(k_hbm, ks, k_sem, h).start()
        for h in range(heads):
            load(v_hbm, vs, v_sem, h).start()

        lane = lax.broadcasted_iota(jnp.int32, (1, 128), 1)
        slots = nz // id_rows
        slot = 128 // slots
        small[0].wait()
        ids = ids_ref[...]
        ids = jnp.concatenate([ids[j : j + 1] for j in range(ids.shape[0])] * slots, axis=1)
        idbs[...] = jnp.where(lax.div(lane, slot) == lax.rem(z, slots), ids, 0)
        idbr[z] = idbs[...]

        def scores(h):
            base = h * groups * 128
            q = jnp.concatenate(
                [q_ref[:, base + g * 128 : base + (g + 1) * 128] for g in range(groups)], axis=0
            )
            s_ref[h] = dot_nt(q, ks[h]) * scaling

        pl.semaphore_wait(barrier, na - 1 + nz - 1)
        send(z_dev, order_z, lambda t: idbs, idbr, z, b_send, b_recv)
        for r in small[1:]:
            r.wait()
        wait_bytes(ks, heads, k_sem)
        for h in range(heads):
            scores(h)

        cols = pl.multiple_of(a * width, width)
        head_cols = pl.multiple_of(lax.div(a, per_head) * 128, 128)
        q_own = q_ref[:, pl.ds(cols, width)]
        q_own = jnp.concatenate(
            [q_own[:, i * 128 : (i + 1) * 128] for i in range(width // 128)], axis=0
        )
        pad = jnp.zeros((128 - drafts, 128), BF16)
        kf = jnp.concatenate([nk_ref[:, pl.ds(head_cols, 128)], pad], axis=0)
        vf = jnp.concatenate([nv_ref[:, pl.ds(head_cols, 128)], pad], axis=0)
        sf = dot_nt(q_own, kf) * scaling
        pos = lax.rem(lax.broadcasted_iota(jnp.int32, sf.shape, 0), drafts)
        ok = lax.broadcasted_iota(jnp.int32, sf.shape, 1) <= pos
        sf = jnp.where(ok, sf, FLOOR)
        mf = jnp.max(sf, axis=1, keepdims=True)
        pf = jnp.where(ok, jnp.exp(sf - mf), 0.0).astype(BF16)
        tf = jnp.sum(pf.astype(F32), axis=1, keepdims=True)
        of = dot_nn(pf, vf) / tf
        lf = flip(jnp.broadcast_to(mf + jnp.log(tf), (block_rows, 128)))[0:1]

        key_page = lax.div(lax.broadcasted_iota(jnp.int32, (128, tokens), 1), page_tokens)
        row_page = lax.broadcasted_iota(jnp.int32, (128, tokens), 0)
        ex[...] = (key_page == row_page).astype(F32).astype(BF16)

        wait_bytes(idbr, nz - 1, b_recv)
        for r in range(id_rows):
            joined = idbr[r * slots]
            for i in range(r * slots + 1, (r + 1) * slots):
                joined = joined + idbr[i]
            idas[r] = joined
            idar[x * nc + c, r] = joined
        send(plane_dev, order_plane, lambda t: idas, idar, x * nc + c, a_send, a_recv)
        wait_bytes(vs, heads, v_sem)
        wait_bytes(idar, nx * nc - 1, a_recv)

        local = jnp.concatenate(
            [idar[i, r] for i in range(nx * nc) for r in range(id_rows)], axis=0
        )
        local = local - ((z * nx + x) * nc + c) * pages
        counts = [
            jnp.sum((local == p).astype(F32), axis=0, keepdims=True) for p in range(pages)
        ]
        counts.append(jnp.zeros((128 - pages, 128), F32))
        counts = jnp.concatenate(counts, axis=0).astype(BF16)
        lane_head = lax.rem(lax.broadcasted_iota(jnp.int32, (heads, 128), 1), heads)
        pick = (lane_head == lax.broadcasted_iota(jnp.int32, (heads, 128), 0)).astype(F32).astype(BF16)
        picked = dot_nt(pick, counts).astype(BF16)
        usable = dot_nn(picked, ex[...])

        lanes = lax.broadcasted_iota(jnp.int32, (block_rows, 128), 1)
        stats = jnp.zeros((block_rows, 128), F32)
        for h in range(heads):
            s = jnp.where(usable[h : h + 1] > 0.5, s_ref[h], FLOOR)
            top = jnp.max(s, axis=1, keepdims=True)
            offset = jnp.where(top > 0.5 * FLOOR, top, 0.0)
            p = jnp.exp(s - offset).astype(BF16)
            total = jnp.sum(p.astype(F32), axis=1, keepdims=True)
            safe = jnp.maximum(total, 0.5)
            o = dot_nn(p, vs[h]) / safe
            lse = jnp.where(total > 0.0, offset + jnp.log(safe), FLOOR)
            for i in range(per_head):
                part = slice(i * block_rows, (i + 1) * block_rows)
                o1s[h * per_head + i] = o[part].astype(BF16)
                stats = jnp.where(lanes == h * per_head + i, lse[part], stats)
        stats = flip(stats)
        for i in range(na):
            l1s[i] = stats[i : i + 1]
        l1r[a] = l1s[a]
        send(a_dev, order_a, lambda t: l1s.at[t], l1r, a, l1_send, l1_recv)
        send(a_dev, order_a, lambda t: o1s.at[t], o1r, a, o1_send, o1_recv)
        o1r[a] = o1s[a]
        wait_bytes(l1r, na - 1, l1_recv)
        w, lse = merge_weights(rows_of(l1r, na))
        w = flip(w)[0:block_rows]
        l2s[...] = lse
        l2r[b] = lse
        send_pairs(l2s, l2r, l2_send, l2_recv)
        wait_bytes(o1r, na - 1, o1_recv)
        o = w[:, 0:1] * o1r[0].astype(F32)
        for i in range(1, na):
            o = o + w[:, i : i + 1] * o1r[i].astype(F32)
        o = o.astype(BF16)
        o2s[...] = o
        o2r[b] = o
        send_pairs(o2s, o2r, o2_send, o2_recv)
        wait_bytes(l2r, nb - 1, l2_recv)
        w, _ = merge_weights(jnp.concatenate([lf, rows_of(l2r, nb)], axis=0))
        w = flip(w)[0:block_rows]
        o = w[:, 0:1] * of
        wait_bytes(o2r, nb - 1, o2_recv)
        for i in range(nb):
            o = o + w[:, i + 1 : i + 2] * o2r[i].astype(F32)
        o = o.astype(BF16)
        block = jnp.concatenate(
            [o[i * drafts : (i + 1) * drafts] for i in range(width // 128)], axis=1
        )
        fs[...] = block
        fr[a] = block
        send_final(fs, fr, f_send, f_recv)
        wait_bytes(fr, na - 1, f_recv)
        for i in range(na):
            out_ref[:, i * width : (i + 1) * width] = fr[i]
        wait_bytes(idbr, nz - 1, b_send)
        wait_bytes(idar, nx * nc - 1, a_send)
        wait_bytes(o1r, na - 1, o1_send)
        wait_bytes(l1r, na - 1, l1_send)
        wait_bytes(o2r, nb - 1, o2_send)
        wait_bytes(l2r, nb - 1, l2_send)
        wait_bytes(fr, na - 1, f_send)

    dma = pltpu.SemaphoreType.DMA
    span = heads * 128
    rows = heads * groups * drafts // heads
    scratch = [
        pltpu.VMEM((drafts, heads * groups * 128), BF16),
        pltpu.VMEM((ids_each // heads, heads), jnp.int32),
        pltpu.VMEM((drafts, span), BF16),
        pltpu.VMEM((drafts, span), BF16),
        dma((4,)),
        pltpu.VMEM((heads, tokens, 128), BF16),
        pltpu.VMEM((heads, tokens, 128), BF16),
        pltpu.VMEM((heads, rows, tokens), F32),
        pltpu.VMEM((1, 128), jnp.int32),
        pltpu.VMEM((nz, 1, 128), jnp.int32),
        pltpu.VMEM((id_rows, 1, 128), jnp.int32),
        pltpu.VMEM((nx * nc, id_rows, 1, 128), jnp.int32),
        pltpu.VMEM((na, block_rows, 128), BF16),
        pltpu.VMEM((na, 1, 128), F32),
        pltpu.VMEM((na, block_rows, 128), BF16),
        pltpu.VMEM((na, 1, 128), F32),
        pltpu.VMEM((block_rows, 128), BF16),
        pltpu.VMEM((1, 128), F32),
        pltpu.VMEM((nb, block_rows, 128), BF16),
        pltpu.VMEM((nb, 1, 128), F32),
        pltpu.VMEM((drafts, width), BF16),
        pltpu.VMEM((na, drafts, width), BF16),
        pltpu.VMEM((128, tokens), BF16),
        *[dma] * 16,
    ]
    vmem = pl.BlockSpec(memory_space=pltpu.VMEM)
    hbm = pl.BlockSpec(memory_space=pltpu.HBM)
    return pl.pallas_call(
        kernel,
        out_shape=jax.ShapeDtypeStruct((drafts, heads * groups * 128), BF16),
        in_specs=[hbm] * 6,
        out_specs=vmem,
        scratch_shapes=scratch,
        compiler_params=pltpu.CompilerParams(
            collective_id=0, has_side_effects=True, vmem_limit_bytes=32 * 1024 * 1024
        ),
    )


def solution(mesh):
    nz, nx, nc = 16, 4, 2
    torus = Mesh(
        mesh.devices.reshape(mesh.shape["grp"], nz, nx, nc), ("grp", "page_0", "page_1", "page_2")
    )

    def on_device(queries, key_cache, value_cache, new_keys, new_values, chosen):
        pages, page_tokens, span = key_cache.shape
        heads = chosen.shape[0]
        drafts = queries.shape[0]
        groups = queries.shape[1] // span
        call = make_kernel(
            nz, nx, nc, heads, chosen.size, pages * page_tokens, page_tokens, drafts, groups,
            (span // heads) ** (-0.5),
        )
        return call(
            *[
                pltpu.with_memory_space_constraint(x, pltpu.HBM)
                for x in (
                    queries, chosen.T, new_keys, new_values,
                    key_cache.reshape(-1, span), value_cache.reshape(-1, span),
                )
            ]
        )

    in_specs = (
        P("grp", None),
        P(GRP_PAGE, None, None),
        P(GRP_PAGE, None, None),
        P("grp", None),
        P("grp", None),
        P("grp", PAGE),
    )
    return jax.shard_map(
        on_device, mesh=torus, in_specs=in_specs, out_specs=P("grp", None), check_vma=False
    )
```

```python
import jax
import jax.numpy as jnp
from jax import lax
from jax.experimental import pallas as pl
from jax.experimental.pallas import tpu as pltpu
from jax.sharding import Mesh
from jax.sharding import PartitionSpec as P

GRP_PAGE = ("grp", "page_0", "page_1", "page_2")
PAGE = GRP_PAGE[1:]
FLOOR = -1e30
F32 = jnp.float32
BF16 = jnp.bfloat16
MESH = pl.DeviceIdType.MESH


def dot_nt(a, b):
    return lax.dot_general(a, b, (((1,), (1,)), ((), ())), preferred_element_type=F32)


def dot_nn(a, b):
    return lax.dot_general(a, b, (((1,), (0,)), ((), ())), preferred_element_type=F32)


def rows_of(ref, count):
    return jnp.concatenate([ref[i] for i in range(count)], axis=0)


def flip(x):
    n = x.shape[0]
    if n < 128:
        x = jnp.concatenate([x, jnp.zeros((128 - n, 128), x.dtype)], axis=0)
    return jnp.transpose(x)


def merge_weights(lse):
    top = jnp.max(lse, axis=0, keepdims=True)
    w = jnp.exp(lse - top)
    total = jnp.sum(w, axis=0, keepdims=True)
    return w / total, top + jnp.log(total)


def far_first(n, ring):
    def key(d):
        return -min(d // ring, (n - d) // ring)

    return sorted(range(1, n), key=key)


def make_kernel(nz, nx, nc, heads, ids_each, tokens, page_tokens, drafts, groups, scaling):
    na = nx * nc * 2
    nb = nz // 2
    pages = tokens // page_tokens
    id_rows = nz * ids_each // 128
    block_rows = heads * groups * drafts // na
    per_head = na // heads
    width = block_rows // drafts * 128

    def kernel(
        q_hbm, ids_hbm, nk_hbm, nv_hbm, k_hbm, v_hbm, out_ref,
        q_ref, ids_ref, nk_ref, nv_ref, small_sem, ks, vs, s_ref, idbs, idbr, idas, idar,
        o1s, l1s, o1r, l1r, o2s, l2s, o2r, l2r, fs, fr, ex,
        k_sem, v_sem, b_send, b_recv, a_send, a_recv,
        o1_send, o1_recv, l1_send, l1_recv,
        o2_send, o2_recv, l2_send, l2_recv, f_send, f_recv,
    ):
        z = lax.axis_index("page_0")
        x = lax.axis_index("page_1")
        c = lax.axis_index("page_2")
        zlow = lax.rem(z, 2)
        b = lax.div(z, 2)
        a = (x * nc + c) * 2 + zlow

        def a_dev(d):
            t = lax.rem(a + d, na)
            u = lax.div(t, 2)
            return t, {
                "page_0": b * 2 + lax.rem(t, 2),
                "page_1": lax.div(u, nc),
                "page_2": lax.rem(u, nc),
            }

        def pair_dev(t):
            return {"page_0": t * 2 + zlow, "page_1": x, "page_2": c}

        def z_dev(d):
            t = lax.rem(z + d, nz)
            return t, {"page_0": t, "page_1": x, "page_2": c}

        def plane_dev(d):
            t = lax.rem(x * nc + c + d, nx * nc)
            return t, {"page_0": z, "page_1": lax.div(t, nc), "page_2": lax.rem(t, nc)}

        order_z = far_first(nz, 1)
        order_plane = far_first(nx * nc, nc)
        order_a = far_first(na, nc * 2)

        def copy(src, dst, ss, rs, dev):
            return pltpu.make_async_remote_copy(
                src_ref=src, dst_ref=dst, send_sem=ss, recv_sem=rs,
                device_id=dev, device_id_type=MESH,
            )

        def send(group, order, src, dst, me, ss, rs):
            for d in order:
                t, dev = group(d)
                copy(src(t), dst.at[me], ss, rs, dev).start()

        def wait_bytes(buf, count, sem):
            part = buf.at[pl.ds(0, count)]
            pltpu.make_async_copy(part, part, sem).wait()

        small = [
            pltpu.make_async_copy(src, dst, small_sem.at[i])
            for i, (src, dst) in enumerate(
                [(ids_hbm, ids_ref), (q_hbm, q_ref), (nk_hbm, nk_ref), (nv_hbm, nv_ref)]
            )
        ]
        small[0].start()

        def after(i, own):
            return i + (i >= own).astype(jnp.int32)

        def send_pairs(src, dst, ss, rs):
            for i in range(nb - 1):
                copy(src, dst.at[b], ss, rs, pair_dev(after(i, b))).start()

        def send_final(src, dst, ss, rs):
            plane = nx * nc
            for i in range(na - 1):
                r = after(i, zlow * plane + x * nc + c)
                u = lax.rem(r, plane)
                dev = {
                    "page_0": b * 2 + lax.div(r, plane),
                    "page_1": lax.div(u, nc),
                    "page_2": lax.rem(u, nc),
                }
                copy(src, dst.at[a], ss, rs, dev).start()

        barrier = pltpu.get_barrier_semaphore()
        for d in order_z:
            pl.semaphore_signal(barrier, inc=1, device_id=z_dev(d)[1], device_id_type=MESH)
        for d in order_a:
            pl.semaphore_signal(barrier, inc=1, device_id=a_dev(d)[1], device_id_type=MESH)

        def load(src, dst, sem, h):
            return pltpu.make_async_copy(src.at[:, pl.ds(h * 128, 128)], dst.at[h], sem)


        lane = lax.broadcasted_iota(jnp.int32, (1, 128), 1)
        slots = nz // id_rows
        slot = 128 // slots
        small[0].wait()
        ids = ids_ref[...]
        ids = jnp.concatenate([ids[j : j + 1] for j in range(ids.shape[0])] * slots, axis=1)
        idbs[...] = jnp.where(lax.div(lane, slot) == lax.rem(z, slots), ids, 0)
        idbr[z] = idbs[...]

        def scores(h):
            base = h * groups * 128
            q = jnp.concatenate(
                [q_ref[:, base + g * 128 : base + (g + 1) * 128] for g in range(groups)], axis=0
            )
            s_ref[h] = dot_nt(q, ks[h]) * scaling

        pl.semaphore_wait(barrier, na - 1 + nz - 1)
        send(z_dev, order_z, lambda t: idbs, idbr, z, b_send, b_recv)
        for r in small[1:]:
            r.start()
        for h in range(heads):
            load(k_hbm, ks, k_sem, h).start()
        for h in range(heads):
            load(v_hbm, vs, v_sem, h).start()
        for r in small[1:]:
            r.wait()
        wait_bytes(ks, heads, k_sem)
        for h in range(heads):
            scores(h)

        cols = pl.multiple_of(a * width, width)
        head_cols = pl.multiple_of(lax.div(a, per_head) * 128, 128)
        q_own = q_ref[:, pl.ds(cols, width)]
        q_own = jnp.concatenate(
            [q_own[:, i * 128 : (i + 1) * 128] for i in range(width // 128)], axis=0
        )
        pad = jnp.zeros((128 - drafts, 128), BF16)
        kf = jnp.concatenate([nk_ref[:, pl.ds(head_cols, 128)], pad], axis=0)
        vf = jnp.concatenate([nv_ref[:, pl.ds(head_cols, 128)], pad], axis=0)
        sf = dot_nt(q_own, kf) * scaling
        pos = lax.rem(lax.broadcasted_iota(jnp.int32, sf.shape, 0), drafts)
        ok = lax.broadcasted_iota(jnp.int32, sf.shape, 1) <= pos
        sf = jnp.where(ok, sf, FLOOR)
        mf = jnp.max(sf, axis=1, keepdims=True)
        pf = jnp.where(ok, jnp.exp(sf - mf), 0.0).astype(BF16)
        tf = jnp.sum(pf.astype(F32), axis=1, keepdims=True)
        of = dot_nn(pf, vf) / tf
        lf = flip(jnp.broadcast_to(mf + jnp.log(tf), (block_rows, 128)))[0:1]

        key_page = lax.div(lax.broadcasted_iota(jnp.int32, (128, tokens), 1), page_tokens)
        row_page = lax.broadcasted_iota(jnp.int32, (128, tokens), 0)
        ex[...] = (key_page == row_page).astype(F32).astype(BF16)

        wait_bytes(idbr, nz - 1, b_recv)
        for r in range(id_rows):
            joined = idbr[r * slots]
            for i in range(r * slots + 1, (r + 1) * slots):
                joined = joined + idbr[i]
            idas[r] = joined
            idar[x * nc + c, r] = joined
        send(plane_dev, order_plane, lambda t: idas, idar, x * nc + c, a_send, a_recv)
        wait_bytes(vs, heads, v_sem)
        wait_bytes(idar, nx * nc - 1, a_recv)

        local = jnp.concatenate(
            [idar[i, r] for i in range(nx * nc) for r in range(id_rows)], axis=0
        )
        local = local - ((z * nx + x) * nc + c) * pages
        counts = [
            jnp.sum((local == p).astype(F32), axis=0, keepdims=True) for p in range(pages)
        ]
        counts.append(jnp.zeros((128 - pages, 128), F32))
        counts = jnp.concatenate(counts, axis=0).astype(BF16)
        lane_head = lax.rem(lax.broadcasted_iota(jnp.int32, (heads, 128), 1), heads)
        pick = (lane_head == lax.broadcasted_iota(jnp.int32, (heads, 128), 0)).astype(F32).astype(BF16)
        picked = dot_nt(pick, counts).astype(BF16)
        usable = dot_nn(picked, ex[...])

        lanes = lax.broadcasted_iota(jnp.int32, (block_rows, 128), 1)
        stats = jnp.zeros((block_rows, 128), F32)
        for h in range(heads):
            s = jnp.where(usable[h : h + 1] > 0.5, s_ref[h], FLOOR)
            top = jnp.max(s, axis=1, keepdims=True)
            offset = jnp.where(top > 0.5 * FLOOR, top, 0.0)
            p = jnp.exp(s - offset).astype(BF16)
            total = jnp.sum(p.astype(F32), axis=1, keepdims=True)
            safe = jnp.maximum(total, 0.5)
            o = dot_nn(p, vs[h]) / safe
            lse = jnp.where(total > 0.0, offset + jnp.log(safe), FLOOR)
            for i in range(per_head):
                part = slice(i * block_rows, (i + 1) * block_rows)
                o1s[h * per_head + i] = o[part].astype(BF16)
                stats = jnp.where(lanes == h * per_head + i, lse[part], stats)
        stats = flip(stats)
        for i in range(na):
            l1s[i] = stats[i : i + 1]
        l1r[a] = l1s[a]
        send(a_dev, order_a, lambda t: l1s.at[t], l1r, a, l1_send, l1_recv)
        send(a_dev, order_a, lambda t: o1s.at[t], o1r, a, o1_send, o1_recv)
        o1r[a] = o1s[a]
        wait_bytes(l1r, na - 1, l1_recv)
        w, lse = merge_weights(rows_of(l1r, na))
        w = flip(w)[0:block_rows]
        l2s[...] = lse
        l2r[b] = lse
        send_pairs(l2s, l2r, l2_send, l2_recv)
        wait_bytes(o1r, na - 1, o1_recv)
        o = w[:, 0:1] * o1r[0].astype(F32)
        for i in range(1, na):
            o = o + w[:, i : i + 1] * o1r[i].astype(F32)
        o = o.astype(BF16)
        o2s[...] = o
        o2r[b] = o
        send_pairs(o2s, o2r, o2_send, o2_recv)
        wait_bytes(l2r, nb - 1, l2_recv)
        w, _ = merge_weights(jnp.concatenate([lf, rows_of(l2r, nb)], axis=0))
        w = flip(w)[0:block_rows]
        o = w[:, 0:1] * of
        wait_bytes(o2r, nb - 1, o2_recv)
        for i in range(nb):
            o = o + w[:, i + 1 : i + 2] * o2r[i].astype(F32)
        o = o.astype(BF16)
        block = jnp.concatenate(
            [o[i * drafts : (i + 1) * drafts] for i in range(width // 128)], axis=1
        )
        fs[...] = block
        fr[a] = block
        send_final(fs, fr, f_send, f_recv)
        wait_bytes(fr, na - 1, f_recv)
        for i in range(na):
            out_ref[:, i * width : (i + 1) * width] = fr[i]
        wait_bytes(idbr, nz - 1, b_send)
        wait_bytes(idar, nx * nc - 1, a_send)
        wait_bytes(o1r, na - 1, o1_send)
        wait_bytes(l1r, na - 1, l1_send)
        wait_bytes(o2r, nb - 1, o2_send)
        wait_bytes(l2r, nb - 1, l2_send)
        wait_bytes(fr, na - 1, f_send)

    dma = pltpu.SemaphoreType.DMA
    span = heads * 128
    rows = heads * groups * drafts // heads
    scratch = [
        pltpu.VMEM((drafts, heads * groups * 128), BF16),
        pltpu.VMEM((ids_each // heads, heads), jnp.int32),
        pltpu.VMEM((drafts, span), BF16),
        pltpu.VMEM((drafts, span), BF16),
        dma((4,)),
        pltpu.VMEM((heads, tokens, 128), BF16),
        pltpu.VMEM((heads, tokens, 128), BF16),
        pltpu.VMEM((heads, rows, tokens), F32),
        pltpu.VMEM((1, 128), jnp.int32),
        pltpu.VMEM((nz, 1, 128), jnp.int32),
        pltpu.VMEM((id_rows, 1, 128), jnp.int32),
        pltpu.VMEM((nx * nc, id_rows, 1, 128), jnp.int32),
        pltpu.VMEM((na, block_rows, 128), BF16),
        pltpu.VMEM((na, 1, 128), F32),
        pltpu.VMEM((na, block_rows, 128), BF16),
        pltpu.VMEM((na, 1, 128), F32),
        pltpu.VMEM((block_rows, 128), BF16),
        pltpu.VMEM((1, 128), F32),
        pltpu.VMEM((nb, block_rows, 128), BF16),
        pltpu.VMEM((nb, 1, 128), F32),
        pltpu.VMEM((drafts, width), BF16),
        pltpu.VMEM((na, drafts, width), BF16),
        pltpu.VMEM((128, tokens), BF16),
        *[dma] * 16,
    ]
    vmem = pl.BlockSpec(memory_space=pltpu.VMEM)
    hbm = pl.BlockSpec(memory_space=pltpu.HBM)
    return pl.pallas_call(
        kernel,
        out_shape=jax.ShapeDtypeStruct((drafts, heads * groups * 128), BF16),
        in_specs=[hbm] * 6,
        out_specs=vmem,
        scratch_shapes=scratch,
        compiler_params=pltpu.CompilerParams(
            collective_id=0, has_side_effects=True, vmem_limit_bytes=32 * 1024 * 1024
        ),
    )


def solution(mesh):
    nz, nx, nc = 16, 4, 2
    torus = Mesh(
        mesh.devices.reshape(mesh.shape["grp"], nz, nx, nc), ("grp", "page_0", "page_1", "page_2")
    )

    def on_device(queries, key_cache, value_cache, new_keys, new_values, chosen):
        pages, page_tokens, span = key_cache.shape
        heads = chosen.shape[0]
        drafts = queries.shape[0]
        groups = queries.shape[1] // span
        call = make_kernel(
            nz, nx, nc, heads, chosen.size, pages * page_tokens, page_tokens, drafts, groups,
            (span // heads) ** (-0.5),
        )
        return call(
            *[
                pltpu.with_memory_space_constraint(x, pltpu.HBM)
                for x in (
                    queries, chosen.T, new_keys, new_values,
                    key_cache.reshape(-1, span), value_cache.reshape(-1, span),
                )
            ]
        )

    in_specs = (
        P("grp", None),
        P(GRP_PAGE, None, None),
        P(GRP_PAGE, None, None),
        P("grp", None),
        P("grp", None),
        P("grp", PAGE),
    )
    return jax.shard_map(
        on_device, mesh=torus, in_specs=in_specs, out_specs=P("grp", None), check_vma=False
    )
```
